512 devices in a mesh: gx: 4 (over y_lo), gy: 128 (over z, y_hi, x, core).
Axes of the slice: x: 4, y: 8 (y_hi: 2, y_lo: 4; y = y_hi * 4 + y_lo), z: 8, core: 2. Of those that a mesh axis runs over, the one named last changes fastest.
Arguments:
- traces: bfloat16 [8, 256, 128, 256], P('gx', 'gy'), may hold values from -6 to 6
- aperture: int32 [8, 256, 9], P('gx', 'gy'), may hold values 0 or 1
- geometry: int32 [8, 256, 3, 128], P('gx', 'gy'), may hold values from 0 to 1023, as said below
- trace_weight: bfloat16 [8, 256, 128], P('gx', 'gy'), may hold values from 0.0087890625 to 0.03515625
- class_weight: float32 [14], replicated, may hold values from 0.3 to 1.5
- traveltime: int32 [14, 256], replicated, may hold values from 0 to 1114
Outputs:
- image: float32 [64, 1024, 256], P('gx', 'gy')
The draws below stay inside these ranges and needn't reach their ends.
Inputs may be any that keep to these rules, and one draw needn't show every extreme that they name: Row 0 of a trace's geometry is an inline midpoint among the 16 image columns of its block's tile, row 1 a crossline midpoint among its tile's 8 columns, row 2 an offset class below 8.
All inputs are finite; a program needn't handle non-finite values. No bound on the sum of `aperture` on one device may be relied on, other than what follows from the above.
Results may differ from the reference program's by a relative error of at most 0.0029.
Values may be sent and summed in bfloat16 or wider, within the bound.
No kernel may reach another device: no remote copies, remote signals or barrier semaphores. Data moves between devices by JAX's collectives and lax.ppermute only.
A program may use at most 64 MiB of HBM per device.

```python
import math
import jax
import jax.numpy as jnp
from jax import lax

NS = 256
NTIME = 256
TR = 128
NH = 8
BB = 2
PX = 16
PY = 8
DSTEP = 8
NC = 14
NBX = 8
NBY = 256
NX = 64
NY = 1024
N_GX = 4
N_GY = 128


def draw_geometry(key, part):
    keys = jax.random.split(jax.random.fold_in(key, 11), 3)
    block_x = jnp.arange(NBX, dtype=jnp.int32)[:, None, None] // BB
    block_y = jnp.arange(NBY, dtype=jnp.int32)[None, :, None] // BB
    inline = block_x * PX + jax.random.randint(keys[0], (NBX, NBY, TR), 0, PX)
    crossline = block_y * PY + jax.random.randint(keys[1], (NBX, NBY, TR), 0, PY)
    offset_class = jax.random.randint(keys[2], (NBX, NBY, TR), 0, NH)
    return jnp.stack([inline, crossline, offset_class], axis=2).astype(jnp.int32)


def draw_traveltime(key, part):
    level = jnp.arange(NC, dtype=jnp.int32)[:, None]
    sample = jnp.arange(NTIME, dtype=jnp.int32)[None, :]
    raw = jax.random.randint(jax.random.fold_in(key, 23), (NC, NTIME), 0, 1 << 20)
    extra = raw % (4 * level + 4)
    return (4 * sample + 3 * level + extra).astype(jnp.int32)


def touch_ends(entries, key, low, high):
    extent = entries.shape
    index_at = [jax.random.randint(jax.random.fold_in(key, axis), (), 0, extent[axis]) for axis in range(len(extent))]
    entries = entries.at[tuple(index_at)].set(low)
    longest = extent.index(max(extent))
    index_at[longest] = (index_at[longest] + 1) % extent[longest]
    return entries.at[tuple(index_at)].set(high)


def levels(stream_key, dims, pieces, least, largest):
    gain = 1.0
    for axis_at, blocks in pieces:
        steps = jax.random.uniform(jax.random.fold_in(jax.random.fold_in(stream_key, 6), axis_at), (blocks,), jnp.float32, least / len(pieces), largest / len(pieces))
        gain = gain * jnp.repeat(jnp.exp(steps), dims[axis_at] // blocks).reshape((-1,) + (1,) * (len(dims) - 1 - axis_at))
    return gain


def scatter_about(stream_key, dims, deviation, bound, cuts=(), kind=jnp.bfloat16):
    result = deviation * jax.random.normal(stream_key, dims, jnp.float32)
    if cuts:
        result = result * levels(stream_key, dims, cuts, -0.22, 0.18)
    return jnp.clip(result, -bound, bound).astype(kind)


def setup_inputs(seed: int = 0) -> dict:
    streams_of = jax.random.split(jax.random.key(seed), 7)
    return {
        "traces": scatter_about(streams_of[0], (NBX, NBY, TR, NS), 1.0, 6.0, ((0, 4), (1, 128))),
        "aperture": touch_ends((jax.random.randint(streams_of[1], (NBX, NBY, 9), 0, 3) < 2).astype(jnp.int32), jax.random.fold_in(streams_of[1], 1), 0, 1),
        "geometry": draw_geometry(jax.random.fold_in(streams_of[6], 71), 0),
        "trace_weight": jnp.clip(jnp.exp(math.log(0.03515625) - 1.3862944 * jax.random.uniform(streams_of[3], (NBX, NBY, TR), jnp.float32) ** levels(streams_of[3], (NBX, NBY, TR), ((0, 4), (1, 128)), -0.2, 0.2)), 0.0087890625, 0.03515625).astype(jnp.bfloat16),
        "class_weight": jnp.clip(jnp.exp(jax.random.uniform(streams_of[4], (NC,), jnp.float32, math.log(0.3), math.log(1.5))), 0.3, 1.5),
        "traveltime": draw_traveltime(jax.random.fold_in(streams_of[6], 71), 0),
    }


def migrate(samples_in, live_weights, geometry, tile_x, tile_y, traveltime, class_weight):
    points = jnp.arange(PX * PY, dtype=jnp.int32)
    point_x = tile_x * PX + points // PY
    point_y = tile_y * PY + points % PY
    distance = jnp.abs(point_x[:, None] - geometry[0][None, :]) + jnp.abs(point_y[:, None] - geometry[1][None, :])
    classes = geometry[2][None, :] + distance // DSTEP
    sample_ids = jnp.arange(NS, dtype=jnp.int32)[:, None]
    samples_wide = samples_in.astype(jnp.float32)

    def add_class(level, image):
        scaled = (live_weights * class_weight[level]).astype(jnp.bfloat16).astype(jnp.float32)
        amplitude = jnp.where(classes == level, scaled[None, :], jnp.float32(0.0))
        stacked = jnp.dot(amplitude, samples_wide, precision=lax.Precision.HIGHEST, preferred_element_type=jnp.float32)
        quarter = traveltime[level]
        first_sample = quarter // 4
        fraction = (quarter % 4).astype(jnp.float32) * 0.25
        interp = jnp.where(sample_ids == first_sample[None, :], 1.0 - fraction[None, :], 0.0) + jnp.where(sample_ids == first_sample[None, :] + 1, fraction[None, :], 0.0)
        return image + jnp.dot(stacked, interp.astype(jnp.float32), precision=lax.Precision.HIGHEST, preferred_element_type=jnp.float32)

    return lax.fori_loop(0, class_weight.shape[0], add_class, jnp.zeros((PX * PY, NTIME), jnp.float32))


def reference(traces, aperture, geometry, trace_weight, class_weight, traveltime):
    padded_traces = jnp.pad(traces, ((BB, BB), (BB, BB), (0, 0), (0, 0)))
    padded_aperture = jnp.pad(aperture, ((BB, BB), (BB, BB), (0, 0)))
    padded_geometry = jnp.pad(geometry, ((BB, BB), (BB, BB), (0, 0), (0, 0)))
    padded_weight = jnp.pad(trace_weight, ((BB, BB), (BB, BB), (0, 0)))
    offset = jnp.arange(3 * BB, dtype=jnp.int32) // BB - 1
    wanted = (1 - offset)[:, None] * 3 + (1 - offset)[None, :]
    choose = (jnp.arange(9, dtype=jnp.int32)[None, None, :] == wanted[:, :, None]).astype(jnp.int32)
    zero_index = jnp.int32(0)

    def one_tile(tile):
        tile_x = (tile // N_GY).astype(jnp.int32)
        tile_y = (tile % N_GY).astype(jnp.int32)
        start_x = (tile_x * BB).astype(jnp.int32)
        start_y = (tile_y * BB).astype(jnp.int32)
        near_traces = lax.dynamic_slice(padded_traces, (start_x, start_y, zero_index, zero_index), (3 * BB, 3 * BB, TR, NS))
        near_aperture = lax.dynamic_slice(padded_aperture, (start_x, start_y, zero_index), (3 * BB, 3 * BB, 9))
        near_geometry = lax.dynamic_slice(padded_geometry, (start_x, start_y, zero_index, zero_index), (3 * BB, 3 * BB, 3, TR))
        near_weight = lax.dynamic_slice(padded_weight, (start_x, start_y, zero_index), (3 * BB, 3 * BB, TR))
        live_block = jnp.sum(near_aperture * choose, axis=2)
        live = jnp.broadcast_to(live_block[:, :, None], near_weight.shape).reshape(-1)
        live_weights = near_weight.reshape(-1).astype(jnp.float32) * live.astype(jnp.float32)
        flat_geometry = jnp.moveaxis(near_geometry, 2, 0).reshape(3, -1)
        return migrate(near_traces.reshape(-1, NS), live_weights, flat_geometry, tile_x, tile_y, traveltime, class_weight)

    tiles = lax.map(one_tile, jnp.arange(N_GX * N_GY, dtype=jnp.int32))
    return tiles.reshape(N_GX, N_GY, PX, PY, NTIME).transpose(0, 2, 1, 3, 4).reshape(NX, NY, NTIME)
```

```python
import jax
import jax.numpy as jnp
from jax import lax
from jax.experimental import pallas as pl
from jax.experimental.pallas import tpu as pltpu
from jax.sharding import PartitionSpec as P

NS = 256
NTIME = 256
PX = 16
PY = 8
DSTEP = 8
TR = 128
NH = 8
NC = 14
COLS = PX * PY
NJ = 4 * TR
NQ = (2 * PX - 1 + 2 * PY - 1) // DSTEP + 1
NQ_MID = (PX - 1 + 2 * PY - 1) // DSTEP + 1
LEVEL = 129.0
BF = jnp.bfloat16
F32 = jnp.float32


def row_of(parts):
    return jnp.concatenate(parts, axis=1)


def geometry_rows(geom_ref):
    def part(kind):
        return row_of([geom_ref[i, kind, k : k + 1, :] for i in range(2) for k in range(2)])

    return part(0), part(1), part(2)


def partners():
    dx = 1 - 2 * (lax.axis_index("gx") % 2)
    dy = 1 - 2 * (lax.axis_index("gy") % 2)
    return dx, dy


def inline_distance(dx, mx):
    px = lax.broadcasted_iota(jnp.int32, (PX, NJ), 0)
    ax = jnp.abs(px + PX * dx - (mx & (PX - 1)))
    ax = (2 * ax - (DSTEP - 1)).astype(F32) * (0.5 / DSTEP)
    ax = jnp.broadcast_to(ax[:, None, :], (PX, PY, NJ)).reshape(COLS, NJ)
    return ax.astype(BF).reshape(COLS // 16, 16, NJ)


def crossline_distance(dy, my):
    py = lax.broadcasted_iota(jnp.int32, (16, NJ), 0) % PY
    ay = jnp.abs(py + PY * dy - (my & (PY - 1)))
    return (ay.astype(F32) * (1.0 / DSTEP)).astype(BF)[None]


def class_scales(h, w_ref, cw_ref):
    w = row_of([w_ref[i, k : k + 1, :] for i in range(2) for k in range(2)]).astype(F32)
    scales = []
    for q in range(NQ):
        cw = jnp.full(h.shape, cw_ref[q], F32)
        for k in range(1, NH):
            cw = jnp.where(h == k, cw_ref[k + q], cw)
        scales.append((w * cw).astype(BF).astype(F32))
    return scales


def live_row(ap_ref, dx, dy):
    entry = (dx + 1) * 3 + dy + 1
    return row_of([jnp.full((1, TR), ap_ref[i, k, entry].astype(F32), F32) for i in range(2) for k in range(2)])


def fill_amplitudes(a_ref, at, ax, ay, scales, live, n_q):
    level = (ax + ay) + jnp.asarray(LEVEL, BF)
    for q in range(n_q):
        scale = jnp.broadcast_to(scales[q] * live, (16, NJ)).astype(BF)[None]
        a = jnp.where(level == jnp.asarray(LEVEL + q, BF), scale, jnp.zeros((), BF))
        a_ref[at : at + COLS, q * NJ : (q + 1) * NJ] = a.reshape(COLS, NJ)


def outer_kernel(ap_ref, cw_ref, traces_ref, geom_ref, w_ref, tt_ref, first_ref, second_ref, tq_ref, t_ref, a_ref):
    mx, my, h = geometry_rows(geom_ref)
    dx, dy = partners()
    sample = lax.broadcasted_iota(jnp.int32, (NS, NTIME), 0).astype(F32)
    traces = traces_ref[...]
    for c in range(NC):
        at = tt_ref[c : c + 1, :].astype(F32) * 0.25
        interp = jnp.maximum(1.0 - jnp.abs(sample - at), 0.0).astype(BF)
        t_ref[c] = jnp.dot(traces, interp, preferred_element_type=F32).astype(BF)
    hf = h.astype(F32)
    for b in range(4):
        rows = slice(b * TR, (b + 1) * TR)
        hcol = jnp.broadcast_to(hf[:, rows], (TR, TR)).T
        hcol = jnp.concatenate([hcol, hcol], axis=1).astype(BF)
        masks = [hcol == jnp.asarray(k, BF) for k in range(NH)]
        for q in range(NQ):
            picked = t_ref[q, rows, :]
            for k in range(1, NH):
                picked = jnp.where(masks[k], t_ref[k + q, rows, :], picked)
            tq_ref[q * NJ + b * TR : q * NJ + (b + 1) * TR, :] = picked
    scales = class_scales(h, w_ref, cw_ref)
    tiles_y = (-dy, dy, 0)
    ays = [crossline_distance(t, my) for t in tiles_y]
    for n, tx in enumerate((dx, -dx)):
        ax = inline_distance(tx, mx)
        for m, ty in enumerate(tiles_y):
            fill_amplitudes(a_ref, (3 * n + m) * COLS, ax, ays[m], scales, live_row(ap_ref, tx, ty), NQ)
    out = jnp.dot(a_ref[...], tq_ref[...], preferred_element_type=F32).astype(BF)
    first_ref[...] = out[: 3 * COLS]
    second_ref[...] = out[3 * COLS :]


def inner_kernel(ap_ref, cw_ref, geom_ref, w_ref, tq_ref, own_ref, a_ref):
    mx, my, h = geometry_rows(geom_ref)
    _, dy = partners()
    scales = class_scales(h, w_ref, cw_ref)
    ax = inline_distance(0, mx)
    for m, ty in enumerate((-dy, dy, 0)):
        fill_amplitudes(a_ref, m * COLS, ax, crossline_distance(ty, my), scales, live_row(ap_ref, 0, ty), NQ_MID)
    own_ref[...] = jnp.dot(a_ref[...], tq_ref[: NQ_MID * NJ, :], preferred_element_type=F32)


def swaps(axis, odd):
    n = lax.axis_size(axis)
    lower = range(1 if odd else 0, n - 1, 2)
    return [p for i in lower for p in ((i, i + 1), (i + 1, i))]


SMEM = pl.BlockSpec(memory_space=pltpu.SMEM)
VMEM = pl.BlockSpec(memory_space=pltpu.VMEM)


def per_device(traces, aperture, geometry, trace_weight, class_weight, traveltime):
    geom = jnp.transpose(geometry, (0, 2, 1, 3))
    first, second, tq = pl.pallas_call(
        outer_kernel,
        out_shape=(
            jax.ShapeDtypeStruct((3 * COLS, NTIME), BF),
            jax.ShapeDtypeStruct((3 * COLS, NTIME), BF),
            jax.ShapeDtypeStruct((NQ * NJ, NTIME), BF),
        ),
        in_specs=[SMEM, SMEM, VMEM, VMEM, VMEM, VMEM],
        out_specs=(VMEM, VMEM, VMEM),
        scratch_shapes=[pltpu.VMEM((NC, NJ, NTIME), BF), pltpu.VMEM((6 * COLS, NQ * NJ), BF)],
        name="outer",
    )(aperture, class_weight, traces.reshape(NJ, NS), geom, trace_weight, traveltime)
    from_first = lax.ppermute(first, "gx", swaps("gx", False))
    from_second = lax.ppermute(second, "gx", swaps("gx", True))
    own = pl.pallas_call(
        inner_kernel,
        out_shape=jax.ShapeDtypeStruct((3 * COLS, NTIME), F32),
        in_specs=[SMEM, SMEM, VMEM, VMEM, VMEM],
        out_specs=VMEM,
        scratch_shapes=[pltpu.VMEM((3 * COLS, NQ_MID * NJ), BF)],
        name="inner",
    )(aperture, class_weight, geom, trace_weight, tq)
    total = own + from_first.astype(F32) + from_second.astype(F32)
    odd = lax.ppermute(total[:COLS].astype(BF), "gy", swaps("gy", True))
    even = lax.ppermute(total[COLS : 2 * COLS].astype(BF), "gy", swaps("gy", False))
    image = total[2 * COLS :] + odd.astype(F32) + even.astype(F32)
    return image.reshape(PX, PY, NTIME)


def solution(mesh):
    return jax.shard_map(
        per_device,
        mesh=mesh,
        in_specs=(
            P("gx", "gy", None, None),
            P("gx", "gy", None),
            P("gx", "gy", None, None),
            P("gx", "gy", None),
            P(),
            P(),
        ),
        out_specs=P("gx", "gy", None),
        check_vma=False,
    )
```

```python
import jax
import jax.numpy as jnp
from jax import lax
from jax.experimental import pallas as pl
from jax.experimental.pallas import tpu as pltpu
from jax.sharding import PartitionSpec as P


NS = 256
NTIME = 256
PX = 16
PY = 8
DSTEP = 8
TR = 128
NH = 8
NC = 14
COLS = PX * PY
NJ = 4 * TR
NQ = (2 * PX - 1 + 2 * PY - 1) // DSTEP + 1
LEVEL = 129.0
BF = jnp.bfloat16
F32 = jnp.float32


NB = 4
ROW_X, ROW_Y, ROW_SCALE, ROW_LIVE = 0, 1, 2, 2 + NQ


def row_of(parts):
    return jnp.concatenate(parts, axis=1)


def blocks(piece):
    return row_of([piece(i, k) for i in range(2) for k in range(2)])


def partners():
    dx = 1 - 2 * (lax.axis_index("gx") % 2)
    dy = 1 - 2 * (lax.axis_index("gy") % 2)
    return dx, dy


def inline_distance(dx, mx):
    px = (lax.broadcasted_iota(jnp.int32, (PX, NJ), 0) + PX * dx).astype(F32)
    ax = (2.0 * jnp.abs(px - mx) - (DSTEP - 1)) * (0.5 / DSTEP)
    ax = jnp.broadcast_to(ax[:, None, :], (PX, PY, NJ)).reshape(COLS, NJ)
    return ax.astype(BF).reshape(COLS // 16, 16, NJ)


def crossline_distance(dy, my):
    py = (lax.broadcasted_iota(jnp.int32, (16, NJ), 0) % PY + PY * dy).astype(F32)
    return (jnp.abs(py - my) * (1.0 / DSTEP)).astype(BF)[None]


def class_scales(h, w, cw_ref):
    scales = []
    for q in range(NQ):
        cw = jnp.full(h.shape, cw_ref[q], F32)
        for k in range(1, NH):
            cw = jnp.where(h == k, cw_ref[k + q], cw)
        scales.append((w * cw).astype(BF).astype(F32))
    return scales


def live_row(ap_ref, dx, dy):
    entry = (dx + 1) * 3 + dy + 1
    return blocks(lambda i, k: jnp.full((1, TR), ap_ref[i, k, entry].astype(F32), F32))


def fill_amplitudes(a_ref, at, ax, ay, scales, live, n_q):
    level = (ax + ay) + jnp.asarray(LEVEL, BF)
    for q in range(n_q):
        scale = jnp.broadcast_to(scales[q] * live, (16, NJ)).astype(BF)[None]
        a = jnp.where(level == jnp.asarray(LEVEL + q, BF), scale, jnp.zeros((), BF))
        a_ref[at : at + COLS, q * NJ : (q + 1) * NJ] = a.reshape(COLS, NJ)


def outer_kernel(
    traces_hbm, geom_hbm, w_hbm, tt_hbm, ap_hbm, cw_hbm,
    first_ref, second_ref, tq_ref, table_ref,
    traces_ref, geom_ref, w_ref, tt_ref, ap_ref, cw_ref, sems, t_ref, a_ref,
):
    pairs = (
        (tt_hbm, tt_ref), (traces_hbm, traces_ref), (geom_hbm, geom_ref),
        (w_hbm, w_ref), (cw_hbm, cw_ref), (ap_hbm, ap_ref),
    )
    copies = [pltpu.make_async_copy(a, b, sems.at[n]) for n, (a, b) in enumerate(pairs)]
    for copy in copies:
        copy.start()
    dx, dy = partners()
    sample = lax.broadcasted_iota(jnp.int32, (NS, NTIME), 0).astype(F32)
    for copy in copies:
        copy.wait()
    h = blocks(lambda i, k: geom_ref[i, 2, k : k + 1, :])
    mx = blocks(lambda i, k: geom_ref[i, 0, k : k + 1, :] & (PX - 1)).astype(F32)
    my = blocks(lambda i, k: geom_ref[i, 1, k : k + 1, :] & (PY - 1)).astype(F32)
    w = blocks(lambda i, k: w_ref[i, k : k + 1, :]).astype(F32)
    scales = class_scales(h, w, cw_ref)
    tiles = ((dx, -dy), (-dx, -dy))
    ay = crossline_distance(-dy, my)
    for n, (tx, ty) in enumerate(tiles):
        fill_amplitudes(a_ref, n * COLS, inline_distance(tx, mx), ay, scales, live_row(ap_ref, tx, ty), NQ)
    traces = traces_ref[...]
    for c in range(NC):
        at = tt_ref[c : c + 1, :].astype(F32) * 0.25
        interp = jnp.maximum(1.0 - jnp.abs(sample - at), 0.0).astype(BF)
        t_ref[c] = jnp.dot(traces, interp, preferred_element_type=F32).astype(BF)
    hf = h.astype(F32)
    for b in range(NB):
        rows = slice(b * TR, (b + 1) * TR)
        hcol = jnp.broadcast_to(hf[:, rows], (TR, TR)).T
        hcol = jnp.concatenate([hcol, hcol], axis=1).astype(BF)
        masks = [hcol == jnp.asarray(k, BF) for k in range(NH)]
        for q in range(NQ):
            picked = t_ref[q, rows, :]
            for k in range(1, NH):
                picked = jnp.where(masks[k], t_ref[k + q, rows, :], picked)
            tq_ref[q * NJ + b * TR : q * NJ + (b + 1) * TR, :] = picked
    out = jnp.dot(a_ref[...], tq_ref[...], preferred_element_type=F32).astype(BF)
    first_ref[...] = out[:COLS]
    second_ref[...] = out[COLS:]
    table_ref[ROW_X : ROW_X + 1, :] = mx
    table_ref[ROW_Y : ROW_Y + 1, :] = my
    for q in range(NQ):
        table_ref[ROW_SCALE + q : ROW_SCALE + q + 1, :] = scales[q]
    for n, (tx, ty, _) in enumerate(inner_tiles(dx, dy)):
        table_ref[ROW_LIVE + n : ROW_LIVE + n + 1, :] = live_row(ap_ref, tx, ty)


def inner_tiles(dx, dy):
    return ((dx, dy, 6), (-dx, dy, 6), (dx, 0, 5), (-dx, 0, 5), (0, -dy, 4), (0, dy, 4), (0, 0, 3))


def inner_kernel(tq_ref, table_ref, slow_ref, pair_ref, own_ref, a_ref):
    dx, dy = partners()
    tiles = inner_tiles(dx, dy)
    mx, my = table_ref[ROW_X : ROW_X + 1, :], table_ref[ROW_Y : ROW_Y + 1, :]
    scales = [table_ref[ROW_SCALE + q : ROW_SCALE + q + 1, :] for q in range(NQ)]
    axs = [inline_distance(t, mx) for t in (dx, -dx, 0)]
    ays = [crossline_distance(t, my) for t in (-dy, dy, 0)]
    which = ((0, 1), (1, 1), (0, 2), (1, 2), (2, 0), (2, 1), (2, 2))
    for n, (_, _, n_q) in enumerate(tiles):
        live = table_ref[ROW_LIVE + n : ROW_LIVE + n + 1, :]
        fill_amplitudes(a_ref, n * COLS, axs[which[n][0]], ays[which[n][1]], scales, live, n_q)

    def part(first, last, low, high):
        a = a_ref[first * COLS : last * COLS, low * NJ : high * NJ]
        return jnp.dot(a, tq_ref[low * NJ : high * NJ, :], preferred_element_type=F32)

    x = part(0, 2, 0, 6)
    pair_ref[: 2 * COLS] = x
    x = part(2, 4, 0, 5)
    own_ref[: 2 * COLS] = x
    x = part(4, 6, 0, 4)
    slow_ref[...] = x[:COLS]
    pair_ref[2 * COLS :] = x[COLS:]
    own_ref[2 * COLS :] = part(6, 7, 0, 3)


def swaps(axis, odd):
    n = lax.axis_size(axis)
    lower = range(1 if odd else 0, n - 1, 2)
    return [p for i in lower for p in ((i, i + 1), (i + 1, i))]


HBM = pl.BlockSpec(memory_space=pltpu.HBM)
VMEM = pl.BlockSpec(memory_space=pltpu.VMEM)
INNER_COST = pl.CostEstimate(flops=2 * 33 * COLS * NJ * NTIME, bytes_accessed=1 << 21, transcendentals=0)
PARAMS = pltpu.CompilerParams(vmem_limit_bytes=24 << 20)


def in_hbm(x):
    return pltpu.with_memory_space_constraint(x, pltpu.HBM)


def per_device(traces, aperture, geometry, trace_weight, class_weight, traveltime):
    geom = jnp.transpose(geometry, (0, 2, 1, 3))
    first, second, tq, table = pl.pallas_call(
        outer_kernel,
        out_shape=(
            jax.ShapeDtypeStruct((COLS, NTIME), BF),
            jax.ShapeDtypeStruct((COLS, NTIME), BF),
            jax.ShapeDtypeStruct((NQ * NJ, NTIME), BF),
            jax.ShapeDtypeStruct((16, NJ), F32),
        ),
        in_specs=[HBM] * 6,
        out_specs=(VMEM,) * 4,
        scratch_shapes=[
            pltpu.VMEM((NJ, NS), BF),
            pltpu.VMEM((2, 3, 2, TR), jnp.int32),
            pltpu.VMEM((2, 2, TR), BF),
            pltpu.VMEM((NC, NTIME), jnp.int32),
            pltpu.SMEM((2, 2, 9), jnp.int32),
            pltpu.SMEM((NC,), F32),
            pltpu.SemaphoreType.DMA((6,)),
            pltpu.VMEM((NC, NJ, NTIME), BF),
            pltpu.VMEM((2 * COLS, NQ * NJ), BF),
        ],
        compiler_params=PARAMS,
        name="outer",
    )(*(in_hbm(x) for x in (traces.reshape(NJ, NS), geom, trace_weight, traveltime, aperture, class_weight)))
    corner_first = lax.ppermute(first, "gx", swaps("gx", False))
    corner_second = lax.ppermute(second, "gx", swaps("gx", True))
    slow, pair, own = pl.pallas_call(
        inner_kernel,
        out_shape=(
            jax.ShapeDtypeStruct((COLS, NTIME), F32),
            jax.ShapeDtypeStruct((3 * COLS, NTIME), F32),
            jax.ShapeDtypeStruct((3 * COLS, NTIME), F32),
        ),
        in_specs=[VMEM] * 2,
        out_specs=(VMEM,) * 3,
        scratch_shapes=[pltpu.VMEM((7 * COLS, NQ * NJ), BF)],
        compiler_params=PARAMS,
        cost_estimate=INNER_COST,
        name="inner",
    )(tq, table)
    near = lax.ppermute(pair, "gy", swaps("gy", False))
    slow = slow + corner_first.astype(F32) + corner_second.astype(F32)
    far = lax.ppermute(slow.astype(BF), "gy", swaps("gy", True))
    own = own + near
    side_first = lax.ppermute(own[:COLS].astype(BF), "gx", swaps("gx", False))
    side_second = lax.ppermute(own[COLS : 2 * COLS].astype(BF), "gx", swaps("gx", True))
    image = own[2 * COLS :] + side_first.astype(F32) + side_second.astype(F32) + far.astype(F32)
    return image.reshape(PX, PY, NTIME)


def solution(mesh):
    return jax.shard_map(
        per_device,
        mesh=mesh,
        in_specs=(
            P("gx", "gy", None, None),
            P("gx", "gy", None),
            P("gx", "gy", None, None),
            P("gx", "gy", None),
            P(),
            P(),
        ),
        out_specs=P("gx", "gy", None),
        check_vma=False,
    )
```

```python
import jax
import jax.numpy as jnp
from jax import lax
from jax.experimental import pallas as pl
from jax.experimental.pallas import tpu as pltpu
from jax.sharding import PartitionSpec as P


NS = 256
NTIME = 256
PX = 16
PY = 8
DSTEP = 8
TR = 128
NH = 8
NC = 14
COLS = PX * PY
NJ = 4 * TR
NQ = (2 * PX - 1 + 2 * PY - 1) // DSTEP + 1
LEVEL = 129.0
BF = jnp.bfloat16
F32 = jnp.float32


NB = 4
NREACH = NH + NQ - 1
PICK_UNROLL = 4
GROUPS = (0, 4, 7, 10, NREACH)
ROW_X, ROW_Y, ROW_SCALE, ROW_LIVE = 0, 1, 2, 2 + NQ


def row_of(parts):
    return jnp.concatenate(parts, axis=1)


def blocks(piece):
    return row_of([piece(i, k) for i in range(2) for k in range(2)])


def partners():
    dx = 1 - 2 * (lax.axis_index("gx") % 2)
    dy = 1 - 2 * (lax.axis_index("gy") % 2)
    return dx, dy


def inline_distance(dx, mx):
    px = (lax.broadcasted_iota(jnp.int32, (PX, NJ), 0) + PX * dx).astype(F32)
    ax = (2.0 * jnp.abs(px - mx) - (DSTEP - 1)) * (0.5 / DSTEP)
    ax = jnp.broadcast_to(ax[:, None, :], (PX, PY, NJ)).reshape(COLS, NJ)
    return ax.astype(BF).reshape(COLS // 16, 16, NJ)


def crossline_distance(dy, my):
    py = (lax.broadcasted_iota(jnp.int32, (16, NJ), 0) % PY + PY * dy).astype(F32)
    return (jnp.abs(py - my) * (1.0 / DSTEP)).astype(BF)[None]


def class_scales(h, w, cw_ref):
    scales = []
    for q in range(NQ):
        cw = jnp.full(h.shape, cw_ref[q], F32)
        for k in range(1, NH):
            cw = jnp.where(h == k, cw_ref[k + q], cw)
        scales.append((w * cw).astype(BF).astype(F32))
    return scales


def live_row(ap_ref, dx, dy):
    entry = (dx + 1) * 3 + dy + 1
    return blocks(lambda i, k: jnp.full((1, TR), ap_ref[i, k, entry].astype(F32), F32))


def fill_amplitudes(a_ref, at, ax, ay, scales, live, n_q):
    level = (ax + ay) + jnp.asarray(LEVEL, BF)
    for q in range(n_q):
        scale = jnp.broadcast_to(scales[q] * live, (16, NJ)).astype(BF)[None]
        a = jnp.where(level == jnp.asarray(LEVEL + q, BF), scale, jnp.zeros((), BF))
        a_ref[at : at + COLS, q * NJ : (q + 1) * NJ] = a.reshape(COLS, NJ)


def outer_kernel(
    traces_hbm, geom_hbm, w_hbm, tt_hbm, ap_hbm, cw_hbm,
    first_ref, corner_ref, tq_ref, table_ref,
    traces_ref, geom_ref, w_ref, tt_ref, ap_ref, cw_ref, sems, class_ref, interp_ref, t_ref, a_ref,
):
    pairs = (
        (tt_hbm, tt_ref), (traces_hbm, traces_ref), (geom_hbm, geom_ref),
        (w_hbm, w_ref), (cw_hbm, cw_ref), (ap_hbm, ap_ref),
    )
    copies = [pltpu.make_async_copy(a, b, sems.at[n]) for n, (a, b) in enumerate(pairs)]
    for copy in copies:
        copy.start()
    dx, dy = partners()
    for copy in copies:
        copy.wait()
    h = blocks(lambda i, k: geom_ref[i, 2, k : k + 1, :])
    mx = blocks(lambda i, k: geom_ref[i, 0, k : k + 1, :] & (PX - 1)).astype(F32)
    my = blocks(lambda i, k: geom_ref[i, 1, k : k + 1, :] & (PY - 1)).astype(F32)
    w = blocks(lambda i, k: w_ref[i, k : k + 1, :]).astype(F32)
    scales = class_scales(h, w, cw_ref)
    hf = h.astype(F32)

    for b in range(NB):
        column = jnp.broadcast_to(hf[:, b * TR : (b + 1) * TR], (TR, TR)).T
        class_ref[b * TR : (b + 1) * TR, :] = column.astype(BF)
    ays = [crossline_distance(t, my) for t in (-dy, 0, dy)]
    axs = [inline_distance(t, mx) for t in (dx, -dx)]
    sample = lax.broadcasted_iota(jnp.int32, (NS, NTIME), 0).astype(F32).astype(BF).reshape(NS // 16, 16, NTIME)
    for n, (tx, ty, n_q) in enumerate(outer_tiles(dx, dy)):
        classes = range(GROUPS[n], GROUPS[n + 1])
        for c in classes:
            quarter = tt_ref[c : c + 1, :]
            whole = jnp.minimum(quarter >> 2, NS).astype(F32)
            part = (quarter & 3).astype(F32) * 0.25
            whole = jnp.broadcast_to(whole, (16, NTIME)).astype(BF)[None]
            part = jnp.broadcast_to(part, (16, NTIME)).astype(BF)[None]
            away = jnp.abs((sample - whole) - part)
            interp = jnp.maximum(jnp.asarray(1.0, BF) - away, jnp.asarray(0.0, BF))
            interp_ref[:, c * NTIME : (c + 1) * NTIME] = interp.reshape(NS, NTIME)
        lanes = slice(classes[0] * NTIME, (classes[-1] + 1) * NTIME)
        t_ref[:, lanes] = jnp.dot(traces_ref[...], interp_ref[:, lanes], preferred_element_type=F32).astype(BF)
        fill_amplitudes(a_ref, n * COLS, axs[n // 3], ays[n % 3], scales, live_row(ap_ref, tx, ty), n_q)

    def pick(n, carry):
        rows = pl.ds(pl.multiple_of(n * 16, 16), 16)
        k = class_ref[rows, :]
        bit4 = k >= jnp.asarray(4.0, BF)
        k = jnp.where(bit4, k - jnp.asarray(4.0, BF), k)
        bit2 = k >= jnp.asarray(2.0, BF)
        k = jnp.where(bit2, k - jnp.asarray(2.0, BF), k)
        bit1 = k >= jnp.asarray(1.0, BF)
        for lane in (0, 128):
            t = [t_ref[rows, c * NTIME + lane : c * NTIME + lane + 128] for c in range(NREACH)]
            for bit, shift in ((bit1, 1), (bit2, 2), (bit4, 4)):
                t = [jnp.where(bit, t[c + shift], t[c]) for c in range(len(t) - shift)]
            for q in range(NQ):
                tq_ref[pl.ds(pl.multiple_of(q * NJ + n * 16, 16), 16), lane : lane + 128] = t[q]
        return carry

    lax.fori_loop(0, NJ // 16, pick, 0, unroll=PICK_UNROLL)
    for n in range(2):
        rows = slice(2 * n * COLS, 2 * (n + 1) * COLS)
        out = jnp.dot(a_ref[rows, :], tq_ref[...], preferred_element_type=F32).astype(BF)
        if n == 0:
            first_ref[: 2 * COLS] = out
        else:
            first_ref[2 * COLS :] = out[:COLS]
            corner_ref[...] = out[COLS:]
    table_ref[ROW_X : ROW_X + 1, :] = mx
    table_ref[ROW_Y : ROW_Y + 1, :] = my
    for q in range(NQ):
        table_ref[ROW_SCALE + q : ROW_SCALE + q + 1, :] = scales[q]
    for n, (tx, ty, _) in enumerate(inner_tiles(dx, dy)):
        table_ref[ROW_LIVE + n : ROW_LIVE + n + 1, :] = live_row(ap_ref, tx, ty)


def outer_tiles(dx, dy):
    return ((dx, -dy, 6), (dx, 0, 6), (dx, dy, 6), (-dx, -dy, 6))


def inner_tiles(dx, dy):
    return ((-dx, dy, 6), (-dx, 0, 6), (0, -dy, 4), (0, dy, 4), (0, 0, 3))


def inner_kernel(tq_ref, table_ref, slow_ref, second_ref, own_ref, a_ref):
    dx, dy = partners()
    tiles = inner_tiles(dx, dy)
    mx, my = table_ref[ROW_X : ROW_X + 1, :], table_ref[ROW_Y : ROW_Y + 1, :]
    scales = [table_ref[ROW_SCALE + q : ROW_SCALE + q + 1, :] for q in range(NQ)]
    axs = [inline_distance(t, mx) for t in (-dx, 0)]
    ays = [crossline_distance(t, my) for t in (-dy, dy, 0)]
    which = ((0, 1), (0, 2), (1, 0), (1, 1), (1, 2))
    for n, (_, _, n_q) in enumerate(tiles):
        live = table_ref[ROW_LIVE + n : ROW_LIVE + n + 1, :]
        fill_amplitudes(a_ref, n * COLS, axs[which[n][0]], ays[which[n][1]], scales, live, n_q)

    def part(first, last, n_q):
        a = a_ref[first * COLS : last * COLS, : n_q * NJ]
        return jnp.dot(a, tq_ref[: n_q * NJ, :], preferred_element_type=F32)

    x = part(0, 2, 6).astype(BF)
    second_ref[COLS:] = x[:COLS]
    second_ref[:COLS] = x[COLS:]
    x = part(2, 4, 4)
    slow_ref[...] = x[:COLS]
    own_ref[COLS:] = x[COLS:]
    own_ref[:COLS] = part(4, 5, 3)


def swaps(axis, odd):
    n = lax.axis_size(axis)
    lower = range(1 if odd else 0, n - 1, 2)
    return [p for i in lower for p in ((i, i + 1), (i + 1, i))]


HBM = pl.BlockSpec(memory_space=pltpu.HBM)
VMEM = pl.BlockSpec(memory_space=pltpu.VMEM)
INNER_COST = pl.CostEstimate(flops=2 * 23 * COLS * NJ * NTIME, bytes_accessed=1 << 21, transcendentals=0)
PARAMS = pltpu.CompilerParams(vmem_limit_bytes=24 << 20)


def in_hbm(x):
    return pltpu.with_memory_space_constraint(x, pltpu.HBM)


def per_device(traces, aperture, geometry, trace_weight, class_weight, traveltime):
    geom = jnp.transpose(geometry, (0, 2, 1, 3))
    first, corner, tq, table = pl.pallas_call(
        outer_kernel,
        out_shape=(
            jax.ShapeDtypeStruct((3 * COLS, NTIME), BF),
            jax.ShapeDtypeStruct((COLS, NTIME), BF),
            jax.ShapeDtypeStruct((NQ * NJ, NTIME), BF),
            jax.ShapeDtypeStruct((16, NJ), F32),
        ),
        in_specs=[HBM] * 6,
        out_specs=(VMEM,) * 4,
        scratch_shapes=[
            pltpu.VMEM((NJ, NS), BF),
            pltpu.VMEM((2, 3, 2, TR), jnp.int32),
            pltpu.VMEM((2, 2, TR), BF),
            pltpu.VMEM((NC, NTIME), jnp.int32),
            pltpu.SMEM((2, 2, 9), jnp.int32),
            pltpu.SMEM((NC,), F32),
            pltpu.SemaphoreType.DMA((6,)),
            pltpu.VMEM((NJ, TR), BF),
            pltpu.VMEM((NS, NREACH * NTIME), BF),
            pltpu.VMEM((NJ, NREACH * NTIME), BF),
            pltpu.VMEM((4 * COLS, NQ * NJ), BF),
        ],
        compiler_params=PARAMS,
        name="outer",
    )(*(in_hbm(x) for x in (traces.reshape(NJ, NS), geom, trace_weight, traveltime, aperture, class_weight)))
    from_first = lax.ppermute(first, "gx", swaps("gx", False))
    from_corner = lax.ppermute(corner, "gx", swaps("gx", True))
    slow, second, own = pl.pallas_call(
        inner_kernel,
        out_shape=(
            jax.ShapeDtypeStruct((COLS, NTIME), F32),
            jax.ShapeDtypeStruct((2 * COLS, NTIME), BF),
            jax.ShapeDtypeStruct((2 * COLS, NTIME), F32),
        ),
        in_specs=[VMEM] * 2,
        out_specs=(VMEM,) * 3,
        scratch_shapes=[pltpu.VMEM((5 * COLS, NQ * NJ), BF)],
        compiler_params=PARAMS,
        cost_estimate=INNER_COST,
        name="inner",
    )(tq, table)
    from_second = lax.ppermute(second, "gx", swaps("gx", True))
    slow = slow + from_first[:COLS].astype(F32) + from_corner.astype(F32)
    far = lax.ppermute(slow.astype(BF), "gy", swaps("gy", True))
    own = own + from_first[COLS:].astype(F32) + from_second.astype(F32)
    near = lax.ppermute(own[COLS:], "gy", swaps("gy", False))
    image = own[:COLS] + near + far.astype(F32)
    return image.reshape(PX, PY, NTIME)


def solution(mesh):
    return jax.shard_map(
        per_device,
        mesh=mesh,
        in_specs=(
            P("gx", "gy", None, None),
            P("gx", "gy", None),
            P("gx", "gy", None, None),
            P("gx", "gy", None),
            P(),
            P(),
        ),
        out_specs=P("gx", "gy", None),
        check_vma=False,
    )
```

```python
import jax
import jax.numpy as jnp
from jax import lax
from jax.experimental import pallas as pl
from jax.experimental.pallas import tpu as pltpu
from jax.sharding import PartitionSpec as P


NS = 256
NTIME = 256
PX = 16
PY = 8
DSTEP = 8
TR = 128
NH = 8
NC = 14
COLS = PX * PY
NJ = 4 * TR
NQ = (2 * PX - 1 + 2 * PY - 1) // DSTEP + 1
LEVEL = 129.0
BF = jnp.bfloat16
F32 = jnp.float32


NB = 4
NREACH = NH + NQ - 1
PICK_UNROLL = 4
ROW_X, ROW_Y, ROW_SCALE, ROW_LIVE = 0, 1, 2, 2 + NQ


def row_of(parts):
    return jnp.concatenate(parts, axis=1)


def blocks(piece):
    return row_of([piece(i, k) for i in range(2) for k in range(2)])


def down(piece, rows):
    return jnp.concatenate([piece] * (rows // 16), axis=0)


def partners():
    dx = 1 - 2 * (lax.axis_index("gx") % 2)
    dy = 1 - 2 * (lax.axis_index("gy") % 2)
    return dx, dy


def inline_distance(dx, mx):
    px = (lax.broadcasted_iota(jnp.int32, (PX, NJ), 0) + PX * dx).astype(F32)
    ax = (2.0 * jnp.abs(px - mx) - (DSTEP - 1)) * (0.5 / DSTEP)
    ax = jnp.broadcast_to(ax[:, None, :], (PX, PY, NJ)).reshape(COLS, NJ)
    return ax.astype(BF)


def crossline_distance(dy, my):
    py = (lax.broadcasted_iota(jnp.int32, (16, NJ), 0) % PY + PY * dy).astype(F32)
    return down((jnp.abs(py - my) * (1.0 / DSTEP)).astype(BF), COLS)


def class_scales(h, w, cw_ref):
    scales = []
    for q in range(NQ):
        cw = jnp.full(h.shape, cw_ref[q], F32)
        for k in range(1, NH):
            cw = jnp.where(h == k, cw_ref[k + q], cw)
        scales.append((w * cw).astype(BF).astype(F32))
    return scales


def live_row(ap_ref, dx, dy):
    entry = (dx + 1) * 3 + dy + 1
    return blocks(lambda i, k: jnp.full((1, TR), ap_ref[i, k, entry].astype(F32), F32))


def amplitude(level, scales, lives, q):
    scale = [down(jnp.broadcast_to(scales[q] * live, (16, NJ)).astype(BF), COLS) for live in lives]
    return jnp.where(level == jnp.asarray(LEVEL + q, BF), jnp.concatenate(scale, axis=0), jnp.zeros((), BF))


def stacked(tq_ref, level, scales, lives, n_q):
    out = jnp.zeros((len(lives) * COLS, NTIME), F32)
    for q in range(n_q):
        a = amplitude(level, scales, lives, q)
        out = out + jnp.dot(a, tq_ref[q * NJ : (q + 1) * NJ, :], preferred_element_type=F32)
    return out


def outer_kernel(
    traces_hbm, geom_hbm, w_hbm, tt_hbm, ap_hbm, cw_hbm,
    first_ref, corner_ref, tq_ref, table_ref,
    traces_ref, geom_ref, w_ref, tt_ref, ap_ref, cw_ref, sems, class_ref, t_ref, level_ref,
):
    pairs = (
        (traces_hbm, traces_ref), (geom_hbm, geom_ref), (tt_hbm, tt_ref),
        (w_hbm, w_ref), (cw_hbm, cw_ref), (ap_hbm, ap_ref),
    )
    copies = [pltpu.make_async_copy(a, b, sems.at[n]) for n, (a, b) in enumerate(pairs)]
    for copy in copies:
        copy.start()
    dx, dy = partners()
    for copy in copies[1:]:
        copy.wait()
    h = blocks(lambda i, k: geom_ref[i, 2, k : k + 1, :])
    mx = blocks(lambda i, k: geom_ref[i, 0, k : k + 1, :] & (PX - 1)).astype(F32)
    my = blocks(lambda i, k: geom_ref[i, 1, k : k + 1, :] & (PY - 1)).astype(F32)
    w = blocks(lambda i, k: w_ref[i, k : k + 1, :]).astype(F32)
    table_ref[ROW_X : ROW_X + 1, :] = mx
    table_ref[ROW_Y : ROW_Y + 1, :] = my
    for q, scale in enumerate(class_scales(h, w, cw_ref)):
        table_ref[ROW_SCALE + q : ROW_SCALE + q + 1, :] = scale
    tiles = outer_tiles(dx, dy)
    for n, (tx, ty) in enumerate(inner_tiles(dx, dy) + tiles):
        table_ref[ROW_LIVE + n : ROW_LIVE + n + 1, :] = live_row(ap_ref, tx, ty)
    hf = h.astype(F32)
    for b in range(NB):
        column = jnp.broadcast_to(hf[:, b * TR : (b + 1) * TR], (TR, TR)).T
        class_ref[b * TR : (b + 1) * TR, :] = jnp.concatenate([column, column], axis=1).astype(BF)
    ays = [crossline_distance(t, my) for t in (-dy, 0, dy)]
    axs = [inline_distance(t, mx) for t in (dx, -dx)]
    which = ((0, 0), (0, 1), (0, 2), (1, 0))
    for n in range(len(tiles)):
        x, y = which[n]
        level_ref[n * COLS : (n + 1) * COLS, :] = axs[x] + ays[y] + jnp.asarray(LEVEL, BF)
    copies[0].wait()
    sample = lax.broadcasted_iota(jnp.int32, (NS, NTIME), 0).astype(F32).astype(BF)
    for c in range(NREACH):
        quarter = tt_ref[c : c + 1, :]
        whole = jnp.minimum(quarter >> 2, NS).astype(F32)
        part = (quarter & 3).astype(F32) * 0.25
        whole = down(jnp.broadcast_to(whole, (16, NTIME)).astype(BF), NS)
        part = down(jnp.broadcast_to(part, (16, NTIME)).astype(BF), NS)
        away = jnp.abs((sample - whole) - part)
        interp = jnp.maximum(jnp.asarray(1.0, BF) - away, jnp.asarray(0.0, BF))
        lanes = slice(c * NTIME, (c + 1) * NTIME)
        for n in range(2):
            rows = slice(n * (NJ // 2), (n + 1) * (NJ // 2))
            t_ref[rows, lanes] = jnp.dot(traces_ref[rows, :], interp, preferred_element_type=F32).astype(BF)

    def pick(n, carry):
        rows = pl.ds(pl.multiple_of(n * 16, 16), 16)
        k = class_ref[rows, :]
        bit4 = k >= jnp.asarray(4.0, BF)
        k = jnp.where(bit4, k - jnp.asarray(4.0, BF), k)
        bit2 = k >= jnp.asarray(2.0, BF)
        k = jnp.where(bit2, k - jnp.asarray(2.0, BF), k)
        bit1 = k >= jnp.asarray(1.0, BF)
        t = [t_ref[rows, c * NTIME : (c + 1) * NTIME] for c in range(NREACH)]
        for bit, shift in ((bit1, 1), (bit2, 2), (bit4, 4)):
            t = [jnp.where(bit, t[c + shift], t[c]) for c in range(len(t) - shift)]
        for q in range(NQ):
            tq_ref[pl.ds(pl.multiple_of(q * NJ + n * 16, 16), 16), :] = t[q]
        return carry

    lax.fori_loop(0, NJ // 16, pick, 0, unroll=PICK_UNROLL)
    _, _, scales, lives = table_rows(table_ref)
    lives = lives[len(inner_tiles(dx, dy)) :]
    sums = []
    for low, high in ((0, 2), (2, 4)):
        level = level_ref[low * COLS : high * COLS, :]
        sums.append(stacked(tq_ref, level, scales, lives[low:high], NQ).astype(BF))
    first_ref[: 2 * COLS] = sums[0]
    first_ref[2 * COLS :] = sums[1][:COLS]
    corner_ref[...] = sums[1][COLS:]


def outer_tiles(dx, dy):
    return ((dx, -dy), (dx, 0), (dx, dy), (-dx, -dy))


def inner_tiles(dx, dy):
    return ((-dx, 0), (-dx, dy), (0, 0), (0, dy), (0, -dy))


def table_rows(table_ref):
    mx, my = table_ref[ROW_X : ROW_X + 1, :], table_ref[ROW_Y : ROW_Y + 1, :]
    scales = [table_ref[ROW_SCALE + q : ROW_SCALE + q + 1, :] for q in range(NQ)]
    return mx, my, scales, [table_ref[ROW_LIVE + n : ROW_LIVE + n + 1, :] for n in range(9)]


def side_kernel(tq_ref, table_ref, second_ref, slow_ref):
    dx, dy = partners()
    mx, my, scales, lives = table_rows(table_ref)
    ax = inline_distance(-dx, mx)
    levels = [ax + crossline_distance(ty, my) + jnp.asarray(LEVEL, BF) for ty in (0, dy)]
    for n, level in enumerate(levels):
        out = stacked(tq_ref, level, scales, lives[n : n + 1], NQ)
        second_ref[n * COLS : (n + 1) * COLS, :] = out.astype(BF)
    level = inline_distance(0, mx) + crossline_distance(-dy, my) + jnp.asarray(LEVEL, BF)
    slow_ref[...] = stacked(tq_ref, level, scales, lives[4:5], 4)


def own_kernel(tq_ref, table_ref, own_ref):
    _, dy = partners()
    mx, my, scales, lives = table_rows(table_ref)
    ax = inline_distance(0, mx)
    for n, ty in enumerate((0, dy)):
        level = ax + crossline_distance(ty, my) + jnp.asarray(LEVEL, BF)
        own_ref[n * COLS : (n + 1) * COLS, :] = stacked(tq_ref, level, scales, lives[2 + n : 3 + n], 3 + n)


def swaps(axis, odd):
    n = lax.axis_size(axis)
    lower = range(1 if odd else 0, n - 1, 2)
    return [p for i in lower for p in ((i, i + 1), (i + 1, i))]


HBM = pl.BlockSpec(memory_space=pltpu.HBM)
VMEM = pl.BlockSpec(memory_space=pltpu.VMEM)
LATER_COST = pl.CostEstimate(flops=2 * 7 * COLS * NJ * NTIME, bytes_accessed=1 << 21, transcendentals=0)
PARAMS = pltpu.CompilerParams(vmem_limit_bytes=24 << 20)


def in_hbm(x):
    return pltpu.with_memory_space_constraint(x, pltpu.HBM)


def later_tiles(kernel, dtypes, tq, table):
    return pl.pallas_call(
        kernel,
        out_shape=tuple(jax.ShapeDtypeStruct(((2 - n) * COLS, NTIME), t) for n, t in enumerate(dtypes)),
        in_specs=[VMEM] * 2,
        out_specs=(VMEM,) * len(dtypes),
        compiler_params=PARAMS,
        cost_estimate=LATER_COST,
    )(tq, table)


def per_device(traces, aperture, geometry, trace_weight, class_weight, traveltime):
    geom = jnp.transpose(geometry, (0, 2, 1, 3))
    first, corner, tq, table = pl.pallas_call(
        outer_kernel,
        out_shape=(
            jax.ShapeDtypeStruct((3 * COLS, NTIME), BF),
            jax.ShapeDtypeStruct((COLS, NTIME), BF),
            jax.ShapeDtypeStruct((NQ * NJ, NTIME), BF),
            jax.ShapeDtypeStruct((24, NJ), F32),
        ),
        in_specs=[HBM] * 6,
        out_specs=(VMEM,) * 4,
        scratch_shapes=[
            pltpu.VMEM((NJ, NS), BF),
            pltpu.VMEM((2, 3, 2, TR), jnp.int32),
            pltpu.VMEM((2, 2, TR), BF),
            pltpu.VMEM((NC, NTIME), jnp.int32),
            pltpu.SMEM((2, 2, 9), jnp.int32),
            pltpu.SMEM((NC,), F32),
            pltpu.SemaphoreType.DMA((6,)),
            pltpu.VMEM((NJ, NTIME), BF),
            pltpu.VMEM((NJ, NREACH * NTIME), BF),
            pltpu.VMEM((4 * COLS, NJ), BF),
        ],
        compiler_params=PARAMS,
        name="outer",
    )(*(in_hbm(x) for x in (traces.reshape(NJ, NS), geom, trace_weight, traveltime, aperture, class_weight)))
    from_first = lax.ppermute(first, "gx", swaps("gx", False))
    from_corner = lax.ppermute(corner, "gx", swaps("gx", True))
    second, slow = later_tiles(side_kernel, (BF, F32), tq, table)
    from_second = lax.ppermute(second, "gx", swaps("gx", True))
    slow = slow + from_first[:COLS].astype(F32) + from_corner.astype(F32)
    far = lax.ppermute(slow.astype(BF), "gy", swaps("gy", True))
    (own,) = later_tiles(own_kernel, (F32,), tq, table)
    own = own + from_first[COLS:].astype(F32) + from_second.astype(F32)
    near = lax.ppermute(own[COLS:], "gy", swaps("gy", False))
    image = own[:COLS] + near + far.astype(F32)
    return image.reshape(PX, PY, NTIME)


def solution(mesh):
    return jax.shard_map(
        per_device,
        mesh=mesh,
        in_specs=(
            P("gx", "gy", None, None),
            P("gx", "gy", None),
            P("gx", "gy", None, None),
            P("gx", "gy", None),
            P(),
            P(),
        ),
        out_specs=P("gx", "gy", None),
        check_vma=False,
    )
```

```python
import jax
import jax.numpy as jnp
from jax import lax
from jax.experimental import pallas as pl
from jax.experimental.pallas import tpu as pltpu
from jax.sharding import PartitionSpec as P


NS = 256
NTIME = 256
PX = 16
PY = 8
DSTEP = 8
TR = 128
NH = 8
NC = 14
COLS = PX * PY
NJ = 4 * TR
NQ = (2 * PX - 1 + 2 * PY - 1) // DSTEP + 1
LEVEL = 129.0
BF = jnp.bfloat16
F32 = jnp.float32


NB = 4
NREACH = NH + NQ - 1
PICK_UNROLL = 4
ROW_X, ROW_Y, ROW_SCALE, ROW_LIVE = 0, 1, 2, 2 + NQ


def row_of(parts):
    return jnp.concatenate(parts, axis=1)


def blocks(piece):
    return row_of([piece(i, k) for i in range(2) for k in range(2)])


def down(piece, rows):
    return jnp.concatenate([piece] * (rows // 16), axis=0)


def partners():
    dx = 1
    dy = 1 - 2 * (lax.axis_index("gy") % 2)
    return dx, dy


def inline_distance(dx, mx):
    px = (lax.broadcasted_iota(jnp.int32, (PX, NJ), 0) + PX * dx).astype(F32)
    ax = (2.0 * jnp.abs(px - mx) - (DSTEP - 1)) * (0.5 / DSTEP)
    ax = jnp.broadcast_to(ax[:, None, :], (PX, PY, NJ)).reshape(COLS, NJ)
    return ax.astype(BF)


def crossline_distance(dy, my):
    py = (lax.broadcasted_iota(jnp.int32, (16, NJ), 0) % PY + PY * dy).astype(F32)
    return down((jnp.abs(py - my) * (1.0 / DSTEP)).astype(BF), COLS)


def class_scales(h, w, cw_ref):
    scales = []
    for q in range(NQ):
        cw = jnp.full(h.shape, cw_ref[q], F32)
        for k in range(1, NH):
            cw = jnp.where(h == k, cw_ref[k + q], cw)
        scales.append((w * cw).astype(BF).astype(F32))
    return scales


def live_row(ap_ref, dx, dy):
    entry = (dx + 1) * 3 + dy + 1
    return blocks(lambda i, k: jnp.full((1, TR), ap_ref[i, k, entry].astype(F32), F32))


def amplitude(level, scales, lives, q):
    scale = [down(jnp.broadcast_to(scales[q] * live, (16, NJ)).astype(BF), COLS) for live in lives]
    return jnp.where(level == jnp.asarray(LEVEL + q, BF), jnp.concatenate(scale, axis=0), jnp.zeros((), BF))


def stacked(tq_ref, level, scales, lives, n_q):
    out = jnp.zeros((len(lives) * COLS, NTIME), F32)
    for q in range(n_q):
        a = amplitude(level, scales, lives, q)
        out = out + jnp.dot(a, tq_ref[q * NJ : (q + 1) * NJ, :], preferred_element_type=F32)
    return out


def outer_kernel(
    traces_hbm, geom_hbm, w_hbm, tt_hbm, ap_hbm, cw_hbm,
    first_ref, corner_ref, tq_ref, table_ref,
    traces_ref, geom_ref, w_ref, tt_ref, ap_ref, cw_ref, sems, class_ref, t_ref, level_ref,
):
    pairs = (
        (traces_hbm, traces_ref), (geom_hbm, geom_ref), (tt_hbm, tt_ref),
        (w_hbm, w_ref), (cw_hbm, cw_ref), (ap_hbm, ap_ref),
    )
    copies = [pltpu.make_async_copy(a, b, sems.at[n]) for n, (a, b) in enumerate(pairs)]
    for copy in copies:
        copy.start()
    dx, dy = partners()
    for copy in copies[1:]:
        copy.wait()
    h = blocks(lambda i, k: geom_ref[i, 2, k : k + 1, :])
    mx = blocks(lambda i, k: geom_ref[i, 0, k : k + 1, :] & (PX - 1)).astype(F32)
    my = blocks(lambda i, k: geom_ref[i, 1, k : k + 1, :] & (PY - 1)).astype(F32)
    w = blocks(lambda i, k: w_ref[i, k : k + 1, :]).astype(F32)
    table_ref[ROW_X : ROW_X + 1, :] = mx
    table_ref[ROW_Y : ROW_Y + 1, :] = my
    for q, scale in enumerate(class_scales(h, w, cw_ref)):
        table_ref[ROW_SCALE + q : ROW_SCALE + q + 1, :] = scale
    tiles = outer_tiles(dx, dy)
    for n, (tx, ty) in enumerate(inner_tiles(dx, dy) + tiles):
        table_ref[ROW_LIVE + n : ROW_LIVE + n + 1, :] = live_row(ap_ref, tx, ty)
    hf = h.astype(F32)
    for b in range(NB):
        column = jnp.broadcast_to(hf[:, b * TR : (b + 1) * TR], (TR, TR)).T
        class_ref[b * TR : (b + 1) * TR, :] = jnp.concatenate([column, column], axis=1).astype(BF)
    ays = [crossline_distance(t, my) for t in (-dy, 0, dy)]
    axs = [inline_distance(t, mx) for t in (dx, -dx)]
    which = ((0, 0), (0, 1), (0, 2), (1, 0))
    for n in range(len(tiles)):
        x, y = which[n]
        level_ref[n * COLS : (n + 1) * COLS, :] = axs[x] + ays[y] + jnp.asarray(LEVEL, BF)
    copies[0].wait()
    sample = lax.broadcasted_iota(jnp.int32, (NS, NTIME), 0).astype(F32).astype(BF)
    for c in range(NREACH):
        quarter = tt_ref[c : c + 1, :]
        whole = jnp.minimum(quarter >> 2, NS).astype(F32)
        part = (quarter & 3).astype(F32) * 0.25
        whole = down(jnp.broadcast_to(whole, (16, NTIME)).astype(BF), NS)
        part = down(jnp.broadcast_to(part, (16, NTIME)).astype(BF), NS)
        away = jnp.abs((sample - whole) - part)
        interp = jnp.maximum(jnp.asarray(1.0, BF) - away, jnp.asarray(0.0, BF))
        lanes = slice(c * NTIME, (c + 1) * NTIME)
        for n in range(2):
            rows = slice(n * (NJ // 2), (n + 1) * (NJ // 2))
            t_ref[rows, lanes] = jnp.dot(traces_ref[rows, :], interp, preferred_element_type=F32).astype(BF)

    def pick(n, carry):
        rows = pl.ds(pl.multiple_of(n * 16, 16), 16)
        k = class_ref[rows, :]
        bit4 = k >= jnp.asarray(4.0, BF)
        k = jnp.where(bit4, k - jnp.asarray(4.0, BF), k)
        bit2 = k >= jnp.asarray(2.0, BF)
        k = jnp.where(bit2, k - jnp.asarray(2.0, BF), k)
        bit1 = k >= jnp.asarray(1.0, BF)
        t = [t_ref[rows, c * NTIME : (c + 1) * NTIME] for c in range(NREACH)]
        for bit, shift in ((bit1, 1), (bit2, 2), (bit4, 4)):
            t = [jnp.where(bit, t[c + shift], t[c]) for c in range(len(t) - shift)]
        for q in range(NQ):
            tq_ref[pl.ds(pl.multiple_of(q * NJ + n * 16, 16), 16), :] = t[q]
        return carry

    lax.fori_loop(0, NJ // 16, pick, 0, unroll=PICK_UNROLL)
    _, _, scales, lives = table_rows(table_ref)
    lives = lives[len(inner_tiles(dx, dy)) :]
    sums = []
    for low, high in ((0, 2), (2, 4)):
        level = level_ref[low * COLS : high * COLS, :]
        sums.append(stacked(tq_ref, level, scales, lives[low:high], NQ).astype(BF))
    first_ref[: 2 * COLS] = sums[0]
    first_ref[2 * COLS :] = sums[1][:COLS]
    corner_ref[...] = sums[1][COLS:]


def outer_tiles(dx, dy):
    return ((dx, -dy), (dx, 0), (dx, dy), (-dx, -dy))


def inner_tiles(dx, dy):
    return ((-dx, 0), (-dx, dy), (0, 0), (0, dy), (0, -dy))


def table_rows(table_ref):
    mx, my = table_ref[ROW_X : ROW_X + 1, :], table_ref[ROW_Y : ROW_Y + 1, :]
    scales = [table_ref[ROW_SCALE + q : ROW_SCALE + q + 1, :] for q in range(NQ)]
    return mx, my, scales, [table_ref[ROW_LIVE + n : ROW_LIVE + n + 1, :] for n in range(9)]


def side_kernel(tq_ref, table_ref, second_ref, slow_ref):
    dx, dy = partners()
    mx, my, scales, lives = table_rows(table_ref)
    ax = inline_distance(-dx, mx)
    levels = [ax + crossline_distance(ty, my) + jnp.asarray(LEVEL, BF) for ty in (0, dy)]
    for n, level in enumerate(levels):
        out = stacked(tq_ref, level, scales, lives[n : n + 1], NQ)
        second_ref[n * COLS : (n + 1) * COLS, :] = out.astype(BF)
    level = inline_distance(0, mx) + crossline_distance(-dy, my) + jnp.asarray(LEVEL, BF)
    slow_ref[...] = stacked(tq_ref, level, scales, lives[4:5], 4)


def own_kernel(tq_ref, table_ref, own_ref):
    _, dy = partners()
    mx, my, scales, lives = table_rows(table_ref)
    ax = inline_distance(0, mx)
    for n, ty in enumerate((0, dy)):
        level = ax + crossline_distance(ty, my) + jnp.asarray(LEVEL, BF)
        own_ref[n * COLS : (n + 1) * COLS, :] = stacked(tq_ref, level, scales, lives[2 + n : 3 + n], 3 + n)


def shifts(axis, up):
    n = lax.axis_size(axis)
    return [(i, i + 1) if up else (i + 1, i) for i in range(n - 1)]


def swaps(axis, odd):
    n = lax.axis_size(axis)
    lower = range(1 if odd else 0, n - 1, 2)
    return [p for i in lower for p in ((i, i + 1), (i + 1, i))]


HBM = pl.BlockSpec(memory_space=pltpu.HBM)
VMEM = pl.BlockSpec(memory_space=pltpu.VMEM)
LATER_COST = pl.CostEstimate(flops=2 * 7 * COLS * NJ * NTIME, bytes_accessed=1 << 21, transcendentals=0)
PARAMS = pltpu.CompilerParams(vmem_limit_bytes=24 << 20)


def in_hbm(x):
    return pltpu.with_memory_space_constraint(x, pltpu.HBM)


def later_tiles(kernel, dtypes, tq, table):
    return pl.pallas_call(
        kernel,
        out_shape=tuple(jax.ShapeDtypeStruct(((2 - n) * COLS, NTIME), t) for n, t in enumerate(dtypes)),
        in_specs=[VMEM] * 2,
        out_specs=(VMEM,) * len(dtypes),
        compiler_params=PARAMS,
        cost_estimate=LATER_COST,
    )(tq, table)


def per_device(traces, aperture, geometry, trace_weight, class_weight, traveltime):
    geom = jnp.transpose(geometry, (0, 2, 1, 3))
    first, corner, tq, table = pl.pallas_call(
        outer_kernel,
        out_shape=(
            jax.ShapeDtypeStruct((3 * COLS, NTIME), BF),
            jax.ShapeDtypeStruct((COLS, NTIME), BF),
            jax.ShapeDtypeStruct((NQ * NJ, NTIME), BF),
            jax.ShapeDtypeStruct((24, NJ), F32),
        ),
        in_specs=[HBM] * 6,
        out_specs=(VMEM,) * 4,
        scratch_shapes=[
            pltpu.VMEM((NJ, NS), BF),
            pltpu.VMEM((2, 3, 2, TR), jnp.int32),
            pltpu.VMEM((2, 2, TR), BF),
            pltpu.VMEM((NC, NTIME), jnp.int32),
            pltpu.SMEM((2, 2, 9), jnp.int32),
            pltpu.SMEM((NC,), F32),
            pltpu.SemaphoreType.DMA((6,)),
            pltpu.VMEM((NJ, NTIME), BF),
            pltpu.VMEM((NJ, NREACH * NTIME), BF),
            pltpu.VMEM((4 * COLS, NJ), BF),
        ],
        compiler_params=PARAMS,
        name="outer",
    )(*(in_hbm(x) for x in (traces.reshape(NJ, NS), geom, trace_weight, traveltime, aperture, class_weight)))
    from_first = lax.ppermute(first, "gx", shifts("gx", True))
    from_corner = lax.ppermute(corner, "gx", shifts("gx", False))
    second, slow = later_tiles(side_kernel, (BF, F32), tq, table)
    from_second = lax.ppermute(second, "gx", shifts("gx", False))
    slow = slow + from_first[:COLS].astype(F32) + from_corner.astype(F32)
    far = lax.ppermute(slow.astype(BF), "gy", swaps("gy", True))
    (own,) = later_tiles(own_kernel, (F32,), tq, table)
    own = own + from_first[COLS:].astype(F32) + from_second.astype(F32)
    near = lax.ppermute(own[COLS:], "gy", swaps("gy", False))
    image = own[:COLS] + near + far.astype(F32)
    return image.reshape(PX, PY, NTIME)


def solution(mesh):
    return jax.shard_map(
        per_device,
        mesh=mesh,
        in_specs=(
            P("gx", "gy", None, None),
            P("gx", "gy", None),
            P("gx", "gy", None, None),
            P("gx", "gy", None),
            P(),
            P(),
        ),
        out_specs=P("gx", "gy", None),
        check_vma=False,
    )
```

```python
import jax
import jax.numpy as jnp
from jax import lax
from jax.experimental import pallas as pl
from jax.experimental.pallas import tpu as pltpu
from jax.sharding import PartitionSpec as P


NS = 256
NTIME = 256
PX = 16
PY = 8
DSTEP = 8
TR = 128
NH = 8
NC = 14
COLS = PX * PY
NJ = 4 * TR
NQ = (2 * PX - 1 + 2 * PY - 1) // DSTEP + 1
LEVEL = 129.0
BF = jnp.bfloat16
F32 = jnp.float32


NB = 4
HALF = COLS // 2
NREACH = NH + NQ - 1
PICK_UNROLL = 4
ROW_X, ROW_Y, ROW_SCALE, ROW_LIVE = 0, 1, 2, 2 + NQ


def row_of(parts):
    return jnp.concatenate(parts, axis=1)


def blocks(piece):
    return row_of([piece(i, k) for i in range(2) for k in range(2)])


def down(piece, rows):
    return jnp.concatenate([piece] * (rows // 16), axis=0)


def partners():
    dx = 1
    dy = 1 - 2 * (lax.axis_index("gy") % 2)
    return dx, dy


def inline_distance(first, last, mx):
    px = (lax.broadcasted_iota(jnp.int32, (last - first, NJ), 0) + first).astype(F32)
    ax = (2.0 * jnp.abs(px - mx) - (DSTEP - 1)) * (0.5 / DSTEP)
    ax = jnp.broadcast_to(ax[:, None, :], (last - first, PY, NJ)).reshape((last - first) * PY, NJ)
    return ax.astype(BF)


def near_and_far(dx, mx):
    low = inline_distance(PX * dx, PX * dx + PX // 2, mx)
    high = inline_distance(PX * dx + PX // 2, PX * dx + PX, mx)
    return (low, high) if dx > 0 else (high, low)


def crossline_distance(dy, my):
    py = (lax.broadcasted_iota(jnp.int32, (16, NJ), 0) % PY + PY * dy).astype(F32)
    return (jnp.abs(py - my) * (1.0 / DSTEP)).astype(BF)


def class_scales(h, w, cw_ref):
    scales = []
    for q in range(NQ):
        cw = jnp.full(h.shape, cw_ref[q], F32)
        for k in range(1, NH):
            cw = jnp.where(h == k, cw_ref[k + q], cw)
        scales.append((w * cw).astype(BF).astype(F32))
    return scales


def live_row(ap_ref, dx, dy):
    entry = (dx + 1) * 3 + dy + 1
    return blocks(lambda i, k: jnp.full((1, TR), ap_ref[i, k, entry].astype(F32), F32))


def amplitude(level, scales, lives, q):
    rows = level.shape[0] // len(lives)
    scale = [down(jnp.broadcast_to(scales[q] * live, (16, NJ)).astype(BF), rows) for live in lives]
    return jnp.where(level == jnp.asarray(LEVEL + q, BF), jnp.concatenate(scale, axis=0), jnp.zeros((), BF))


def stacked(tq_ref, level, scales, lives, reach):
    out = jnp.zeros((level.shape[0], NTIME), F32)
    for q in reach:
        a = amplitude(level, scales, lives, q)
        out = out + jnp.dot(a, tq_ref[q * NJ : (q + 1) * NJ, :], preferred_element_type=F32)
    return out


def levels(ax, ay):
    return ax + down(ay, ax.shape[0]) + jnp.asarray(LEVEL, BF)


def outer_kernel(
    traces_hbm, geom_hbm, w_hbm, tt_hbm, ap_hbm, cw_hbm,
    first_ref, corner_ref, tq_ref, table_ref,
    traces_ref, geom_ref, w_ref, tt_ref, ap_ref, cw_ref, sems, class_ref, t_ref, level_ref,
):
    pairs = (
        (traces_hbm, traces_ref), (geom_hbm, geom_ref), (tt_hbm, tt_ref),
        (w_hbm, w_ref), (cw_hbm, cw_ref), (ap_hbm, ap_ref),
    )
    copies = [pltpu.make_async_copy(a, b, sems.at[n]) for n, (a, b) in enumerate(pairs)]
    for copy in copies:
        copy.start()
    dx, dy = partners()
    for copy in copies[1:]:
        copy.wait()
    h = blocks(lambda i, k: geom_ref[i, 2, k : k + 1, :])
    mx = blocks(lambda i, k: geom_ref[i, 0, k : k + 1, :] & (PX - 1)).astype(F32)
    my = blocks(lambda i, k: geom_ref[i, 1, k : k + 1, :] & (PY - 1)).astype(F32)
    w = blocks(lambda i, k: w_ref[i, k : k + 1, :]).astype(F32)
    table_ref[ROW_X : ROW_X + 1, :] = mx
    table_ref[ROW_Y : ROW_Y + 1, :] = my
    for q, scale in enumerate(class_scales(h, w, cw_ref)):
        table_ref[ROW_SCALE + q : ROW_SCALE + q + 1, :] = scale
    tiles = outer_tiles(dx, dy)
    for n, (tx, ty) in enumerate(inner_tiles(dx, dy) + tiles):
        table_ref[ROW_LIVE + n : ROW_LIVE + n + 1, :] = live_row(ap_ref, tx, ty)
    hf = h.astype(F32)
    for b in range(NB):
        column = jnp.broadcast_to(hf[:, b * TR : (b + 1) * TR], (TR, TR)).T
        class_ref[b * TR : (b + 1) * TR, :] = jnp.concatenate([column, column], axis=1).astype(BF)
    ays = [crossline_distance(t, my) for t in (-dy, 0, dy)]
    axs = [near_and_far(t, mx) for t in (dx, -dx)]
    which = ((0, 0), (0, 1), (0, 2), (1, 0))
    for half in range(2):
        for n, (x, y) in enumerate(which):
            at = (4 * half + n) * HALF
            level_ref[at : at + HALF, :] = levels(axs[x][half], ays[y])
    copies[0].wait()
    sample = lax.broadcasted_iota(jnp.int32, (NS, NTIME), 0).astype(F32).astype(BF)
    for c in range(NREACH):
        quarter = tt_ref[c : c + 1, :]
        whole = jnp.minimum(quarter >> 2, NS).astype(F32)
        part = (quarter & 3).astype(F32) * 0.25
        whole = down(jnp.broadcast_to(whole, (16, NTIME)).astype(BF), NS)
        part = down(jnp.broadcast_to(part, (16, NTIME)).astype(BF), NS)
        away = jnp.abs((sample - whole) - part)
        interp = jnp.maximum(jnp.asarray(1.0, BF) - away, jnp.asarray(0.0, BF))
        lanes = slice(c * NTIME, (c + 1) * NTIME)
        for n in range(2):
            rows = slice(n * (NJ // 2), (n + 1) * (NJ // 2))
            t_ref[rows, lanes] = jnp.dot(traces_ref[rows, :], interp, preferred_element_type=F32).astype(BF)

    def pick(n, carry):
        rows = pl.ds(pl.multiple_of(n * 16, 16), 16)
        k = class_ref[rows, :]
        bit4 = k >= jnp.asarray(4.0, BF)
        k = jnp.where(bit4, k - jnp.asarray(4.0, BF), k)
        bit2 = k >= jnp.asarray(2.0, BF)
        k = jnp.where(bit2, k - jnp.asarray(2.0, BF), k)
        bit1 = k >= jnp.asarray(1.0, BF)
        t = [t_ref[rows, c * NTIME : (c + 1) * NTIME] for c in range(NREACH)]
        for bit, shift in ((bit1, 1), (bit2, 2), (bit4, 4)):
            t = [jnp.where(bit, t[c + shift], t[c]) for c in range(len(t) - shift)]
        for q in range(NQ):
            tq_ref[pl.ds(pl.multiple_of(q * NJ + n * 16, 16), 16), :] = t[q]
        return carry

    lax.fori_loop(0, NJ // 16, pick, 0, unroll=PICK_UNROLL)
    _, _, scales, lives = table_rows(table_ref)
    lives = lives[len(inner_tiles(dx, dy)) :]
    near = stacked(tq_ref, level_ref[: 4 * HALF, :], scales, lives, range(NQ - 1)).astype(BF)
    far = stacked(tq_ref, level_ref[4 * HALF :, :], scales, lives, range(1, NQ)).astype(BF)
    for n in range(3):
        rows = slice(n * HALF, (n + 1) * HALF)
        first_ref[n * COLS : n * COLS + HALF, :] = near[rows]
        first_ref[n * COLS + HALF : (n + 1) * COLS, :] = far[rows]
    corner_ref[:HALF, :] = far[3 * HALF :]
    corner_ref[HALF:, :] = near[3 * HALF :]


def outer_tiles(dx, dy):
    return ((dx, -dy), (dx, 0), (dx, dy), (-dx, -dy))


def inner_tiles(dx, dy):
    return ((-dx, 0), (-dx, dy), (0, 0), (0, dy), (0, -dy))


def table_rows(table_ref):
    mx, my = table_ref[ROW_X : ROW_X + 1, :], table_ref[ROW_Y : ROW_Y + 1, :]
    scales = [table_ref[ROW_SCALE + q : ROW_SCALE + q + 1, :] for q in range(NQ)]
    return mx, my, scales, [table_ref[ROW_LIVE + n : ROW_LIVE + n + 1, :] for n in range(9)]


def side_kernel(tq_ref, table_ref, second_ref, slow_ref):
    dx, dy = partners()
    mx, my, scales, lives = table_rows(table_ref)
    halves = near_and_far(-dx, mx)
    ays = [crossline_distance(ty, my) for ty in (0, dy)]
    for half, reach in enumerate((range(NQ - 1), range(1, NQ))):
        level = jnp.concatenate([levels(halves[half], ay) for ay in ays], axis=0)
        out = stacked(tq_ref, level, scales, lives[:2], reach).astype(BF)
        for n in range(2):
            at = n * COLS + (1 - half) * HALF
            second_ref[at : at + HALF, :] = out[n * HALF : (n + 1) * HALF]
    level = levels(inline_distance(0, PX, mx), crossline_distance(-dy, my))
    slow_ref[...] = stacked(tq_ref, level, scales, lives[4:5], range(4))


def own_kernel(tq_ref, table_ref, own_ref):
    _, dy = partners()
    mx, my, scales, lives = table_rows(table_ref)
    ax = inline_distance(0, PX, mx)
    for n, ty in enumerate((0, dy)):
        level = levels(ax, crossline_distance(ty, my))
        own_ref[n * COLS : (n + 1) * COLS, :] = stacked(tq_ref, level, scales, lives[2 + n : 3 + n], range(3 + n))


def shifts(axis, up):
    n = lax.axis_size(axis)
    return [(i, i + 1) if up else (i + 1, i) for i in range(n - 1)]


def swaps(axis, odd):
    n = lax.axis_size(axis)
    lower = range(1 if odd else 0, n - 1, 2)
    return [p for i in lower for p in ((i, i + 1), (i + 1, i))]


HBM = pl.BlockSpec(memory_space=pltpu.HBM)
VMEM = pl.BlockSpec(memory_space=pltpu.VMEM)
LATER_COST = pl.CostEstimate(flops=2 * 7 * COLS * NJ * NTIME, bytes_accessed=1 << 21, transcendentals=0)
PARAMS = pltpu.CompilerParams(vmem_limit_bytes=24 << 20)


def in_hbm(x):
    return pltpu.with_memory_space_constraint(x, pltpu.HBM)


def later_tiles(kernel, dtypes, tq, table):
    return pl.pallas_call(
        kernel,
        out_shape=tuple(jax.ShapeDtypeStruct(((2 - n) * COLS, NTIME), t) for n, t in enumerate(dtypes)),
        in_specs=[VMEM] * 2,
        out_specs=(VMEM,) * len(dtypes),
        compiler_params=PARAMS,
        cost_estimate=LATER_COST,
    )(tq, table)


def per_device(traces, aperture, geometry, trace_weight, class_weight, traveltime):
    geom = jnp.transpose(geometry, (0, 2, 1, 3))
    first, corner, tq, table = pl.pallas_call(
        outer_kernel,
        out_shape=(
            jax.ShapeDtypeStruct((3 * COLS, NTIME), BF),
            jax.ShapeDtypeStruct((COLS, NTIME), BF),
            jax.ShapeDtypeStruct((NQ * NJ, NTIME), BF),
            jax.ShapeDtypeStruct((24, NJ), F32),
        ),
        in_specs=[HBM] * 6,
        out_specs=(VMEM,) * 4,
        scratch_shapes=[
            pltpu.VMEM((NJ, NS), BF),
            pltpu.VMEM((2, 3, 2, TR), jnp.int32),
            pltpu.VMEM((2, 2, TR), BF),
            pltpu.VMEM((NC, NTIME), jnp.int32),
            pltpu.SMEM((2, 2, 9), jnp.int32),
            pltpu.SMEM((NC,), F32),
            pltpu.SemaphoreType.DMA((6,)),
            pltpu.VMEM((NJ, NTIME), BF),
            pltpu.VMEM((NJ, NREACH * NTIME), BF),
            pltpu.VMEM((4 * COLS, NJ), BF),
        ],
        compiler_params=PARAMS,
        name="outer",
    )(*(in_hbm(x) for x in (traces.reshape(NJ, NS), geom, trace_weight, traveltime, aperture, class_weight)))
    from_first = lax.ppermute(first, "gx", shifts("gx", True))
    from_corner = lax.ppermute(corner, "gx", shifts("gx", False))
    second, slow = later_tiles(side_kernel, (BF, F32), tq, table)
    from_second = lax.ppermute(second, "gx", shifts("gx", False))
    slow = slow + from_first[:COLS].astype(F32) + from_corner.astype(F32)
    far = lax.ppermute(slow.astype(BF), "gy", swaps("gy", True))
    (own,) = later_tiles(own_kernel, (F32,), tq, table)
    own = own + from_first[COLS:].astype(F32) + from_second.astype(F32)
    near = lax.ppermute(own[COLS:], "gy", swaps("gy", False))
    image = own[:COLS] + near + far.astype(F32)
    return image.reshape(PX, PY, NTIME)


def solution(mesh):
    return jax.shard_map(
        per_device,
        mesh=mesh,
        in_specs=(
            P("gx", "gy", None, None),
            P("gx", "gy", None),
            P("gx", "gy", None, None),
            P("gx", "gy", None),
            P(),
            P(),
        ),
        out_specs=P("gx", "gy", None),
        check_vma=False,
    )
```

```python
import jax
import jax.numpy as jnp
from jax import lax
from jax.experimental import pallas as pl
from jax.experimental.pallas import tpu as pltpu
from jax.sharding import PartitionSpec as P


NS = 256
NTIME = 256
PX = 16
PY = 8
DSTEP = 8
TR = 128
NH = 8
NC = 14
COLS = PX * PY
NJ = 4 * TR
NQ = (2 * PX - 1 + 2 * PY - 1) // DSTEP + 1
LEVEL = 129.0
BF = jnp.bfloat16
F32 = jnp.float32


NB = 4
HALF = COLS // 2
NREACH = NH + NQ - 1
PICK_UNROLL = 4
ROW_X, ROW_Y, ROW_SCALE, ROW_LIVE = 0, 1, 2, 2 + NQ


def row_of(parts):
    return jnp.concatenate(parts, axis=1)


def blocks(piece):
    return row_of([piece(i, k) for i in range(2) for k in range(2)])


def down(piece, rows):
    return jnp.concatenate([piece] * (rows // 16), axis=0)


def partners():
    dx = 1 - 2 * (lax.axis_index("gx") % 2)
    dy = 1 - 2 * (lax.axis_index("gy") % 2)
    return dx, dy


def inline_distance(first, count, mx):
    px = (lax.broadcasted_iota(jnp.int32, (count, NJ), 0) + first).astype(F32)
    ax = (2.0 * jnp.abs(px - mx) - (DSTEP - 1)) * (0.5 / DSTEP)
    ax = jnp.broadcast_to(ax[:, None, :], (count, PY, NJ)).reshape(count * PY, NJ)
    return ax.astype(BF)


def halves(dx):
    near = (PX // 4) * (1 - dx)
    return near, PX // 2 - near


def near_and_far(dx, mx):
    return [inline_distance(PX * dx + half, PX // 2, mx) for half in halves(dx)]


def half_rows(n, half):
    return pl.ds(pl.multiple_of(n * COLS + half * PY, HALF), HALF)


def crossline_distance(dy, my):
    py = (lax.broadcasted_iota(jnp.int32, (16, NJ), 0) % PY + PY * dy).astype(F32)
    return (jnp.abs(py - my) * (1.0 / DSTEP)).astype(BF)


def class_scales(h, w, cw_ref):
    scales = []
    for q in range(NQ):
        cw = jnp.full(h.shape, cw_ref[q], F32)
        for k in range(1, NH):
            cw = jnp.where(h == k, cw_ref[k + q], cw)
        scales.append((w * cw).astype(BF).astype(F32))
    return scales


def live_row(ap_ref, dx, dy):
    entry = (dx + 1) * 3 + dy + 1
    return blocks(lambda i, k: jnp.full((1, TR), ap_ref[i, k, entry].astype(F32), F32))


def amplitude(level, scales, lives, q):
    rows = level.shape[0] // len(lives)
    scale = [down(jnp.broadcast_to(scales[q] * live, (16, NJ)).astype(BF), rows) for live in lives]
    return jnp.where(level == jnp.asarray(LEVEL + q, BF), jnp.concatenate(scale, axis=0), jnp.zeros((), BF))


def stacked(tq_ref, level, scales, lives, reach):
    out = jnp.zeros((level.shape[0], NTIME), F32)
    for q in reach:
        a = amplitude(level, scales, lives, q)
        out = out + jnp.dot(a, tq_ref[q * NJ : (q + 1) * NJ, :], preferred_element_type=F32)
    return out


def levels(ax, ay):
    return ax + down(ay, ax.shape[0]) + jnp.asarray(LEVEL, BF)


def outer_kernel(
    traces_hbm, geom_hbm, w_hbm, tt_hbm, ap_hbm, cw_hbm,
    first_ref, corner_ref, tq_ref, table_ref,
    traces_ref, geom_ref, w_ref, tt_ref, ap_ref, cw_ref, sems, class_ref, t_ref, level_ref,
):
    pairs = (
        (traces_hbm, traces_ref), (geom_hbm, geom_ref), (tt_hbm, tt_ref),
        (w_hbm, w_ref), (cw_hbm, cw_ref), (ap_hbm, ap_ref),
    )
    copies = [pltpu.make_async_copy(a, b, sems.at[n]) for n, (a, b) in enumerate(pairs)]
    for copy in copies:
        copy.start()
    dx, dy = partners()
    for copy in copies[1:]:
        copy.wait()
    h = blocks(lambda i, k: geom_ref[i, 2, k : k + 1, :])
    mx = blocks(lambda i, k: geom_ref[i, 0, k : k + 1, :] & (PX - 1)).astype(F32)
    my = blocks(lambda i, k: geom_ref[i, 1, k : k + 1, :] & (PY - 1)).astype(F32)
    w = blocks(lambda i, k: w_ref[i, k : k + 1, :]).astype(F32)
    table_ref[ROW_X : ROW_X + 1, :] = mx
    table_ref[ROW_Y : ROW_Y + 1, :] = my
    for q, scale in enumerate(class_scales(h, w, cw_ref)):
        table_ref[ROW_SCALE + q : ROW_SCALE + q + 1, :] = scale
    tiles = outer_tiles(dx, dy)
    for n, (tx, ty) in enumerate(inner_tiles(dx, dy) + tiles):
        table_ref[ROW_LIVE + n : ROW_LIVE + n + 1, :] = live_row(ap_ref, tx, ty)
    hf = h.astype(F32)
    for b in range(NB):
        column = jnp.broadcast_to(hf[:, b * TR : (b + 1) * TR], (TR, TR)).T
        class_ref[b * TR : (b + 1) * TR, :] = jnp.concatenate([column, column], axis=1).astype(BF)
    ays = [crossline_distance(t, my) for t in (-dy, 0, dy)]
    axs = [near_and_far(t, mx) for t in (dx, -dx)]
    which = ((0, 0), (0, 1), (0, 2), (1, 0))
    for half in range(2):
        for n, (x, y) in enumerate(which):
            at = (4 * half + n) * HALF
            level_ref[at : at + HALF, :] = levels(axs[x][half], ays[y])
    copies[0].wait()
    sample = lax.broadcasted_iota(jnp.int32, (NS, NTIME), 0).astype(F32).astype(BF)
    for c in range(NREACH):
        quarter = tt_ref[c : c + 1, :]
        whole = jnp.minimum(quarter >> 2, NS).astype(F32)
        part = (quarter & 3).astype(F32) * 0.25
        whole = down(jnp.broadcast_to(whole, (16, NTIME)).astype(BF), NS)
        part = down(jnp.broadcast_to(part, (16, NTIME)).astype(BF), NS)
        away = jnp.abs((sample - whole) - part)
        interp = jnp.maximum(jnp.asarray(1.0, BF) - away, jnp.asarray(0.0, BF))
        lanes = slice(c * NTIME, (c + 1) * NTIME)
        for n in range(2):
            rows = slice(n * (NJ // 2), (n + 1) * (NJ // 2))
            t_ref[rows, lanes] = jnp.dot(traces_ref[rows, :], interp, preferred_element_type=F32).astype(BF)

    def pick(n, carry):
        rows = pl.ds(pl.multiple_of(n * 16, 16), 16)
        k = class_ref[rows, :]
        bit4 = k >= jnp.asarray(4.0, BF)
        k = jnp.where(bit4, k - jnp.asarray(4.0, BF), k)
        bit2 = k >= jnp.asarray(2.0, BF)
        k = jnp.where(bit2, k - jnp.asarray(2.0, BF), k)
        bit1 = k >= jnp.asarray(1.0, BF)
        t = [t_ref[rows, c * NTIME : (c + 1) * NTIME] for c in range(NREACH)]
        for bit, shift in ((bit1, 1), (bit2, 2), (bit4, 4)):
            t = [jnp.where(bit, t[c + shift], t[c]) for c in range(len(t) - shift)]
        for q in range(NQ):
            tq_ref[pl.ds(pl.multiple_of(q * NJ + n * 16, 16), 16), :] = t[q]
        return carry

    lax.fori_loop(0, NJ // 16, pick, 0, unroll=PICK_UNROLL)
    _, _, scales, lives = table_rows(table_ref)
    lives = lives[len(inner_tiles(dx, dy)) :]
    near = stacked(tq_ref, level_ref[: 4 * HALF, :], scales, lives, range(NQ - 1)).astype(BF)
    far = stacked(tq_ref, level_ref[4 * HALF :, :], scales, lives, range(1, NQ)).astype(BF)
    for out, half in zip((near, far), halves(dx), strict=True):
        for n in range(3):
            first_ref[half_rows(n, half), :] = out[n * HALF : (n + 1) * HALF]
    for out, half in zip((near, far), halves(-dx), strict=True):
        corner_ref[half_rows(0, half), :] = out[3 * HALF :]


def outer_tiles(dx, dy):
    return ((dx, -dy), (dx, 0), (dx, dy), (-dx, -dy))


def inner_tiles(dx, dy):
    return ((-dx, 0), (-dx, dy), (0, 0), (0, dy), (0, -dy))


def table_rows(table_ref):
    mx, my = table_ref[ROW_X : ROW_X + 1, :], table_ref[ROW_Y : ROW_Y + 1, :]
    scales = [table_ref[ROW_SCALE + q : ROW_SCALE + q + 1, :] for q in range(NQ)]
    return mx, my, scales, [table_ref[ROW_LIVE + n : ROW_LIVE + n + 1, :] for n in range(9)]


def side_kernel(tq_ref, table_ref, second_ref, slow_ref):
    dx, dy = partners()
    mx, my, scales, lives = table_rows(table_ref)
    axs = near_and_far(-dx, mx)
    ays = [crossline_distance(ty, my) for ty in (0, dy)]
    for ax, half, reach in zip(axs, halves(-dx), (range(NQ - 1), range(1, NQ)), strict=True):
        level = jnp.concatenate([levels(ax, ay) for ay in ays], axis=0)
        out = stacked(tq_ref, level, scales, lives[:2], reach).astype(BF)
        for n in range(2):
            second_ref[half_rows(n, half), :] = out[n * HALF : (n + 1) * HALF]
    level = levels(inline_distance(0, PX, mx), crossline_distance(-dy, my))
    slow_ref[...] = stacked(tq_ref, level, scales, lives[4:5], range(4))


def own_kernel(tq_ref, table_ref, own_ref):
    _, dy = partners()
    mx, my, scales, lives = table_rows(table_ref)
    ax = inline_distance(0, PX, mx)
    for n, ty in enumerate((0, dy)):
        level = levels(ax, crossline_distance(ty, my))
        own_ref[n * COLS : (n + 1) * COLS, :] = stacked(tq_ref, level, scales, lives[2 + n : 3 + n], range(3 + n))


def swaps(axis, odd):
    n = lax.axis_size(axis)
    lower = range(1 if odd else 0, n - 1, 2)
    return [p for i in lower for p in ((i, i + 1), (i + 1, i))]


HBM = pl.BlockSpec(memory_space=pltpu.HBM)
VMEM = pl.BlockSpec(memory_space=pltpu.VMEM)
LATER_COST = pl.CostEstimate(flops=2 * 7 * COLS * NJ * NTIME, bytes_accessed=1 << 21, transcendentals=0)
PARAMS = pltpu.CompilerParams(vmem_limit_bytes=24 << 20)


def in_hbm(x):
    return pltpu.with_memory_space_constraint(x, pltpu.HBM)


def later_tiles(kernel, dtypes, tq, table):
    return pl.pallas_call(
        kernel,
        out_shape=tuple(jax.ShapeDtypeStruct(((2 - n) * COLS, NTIME), t) for n, t in enumerate(dtypes)),
        in_specs=[VMEM] * 2,
        out_specs=(VMEM,) * len(dtypes),
        compiler_params=PARAMS,
        cost_estimate=LATER_COST,
    )(tq, table)


def per_device(traces, aperture, geometry, trace_weight, class_weight, traveltime):
    geom = jnp.transpose(geometry, (0, 2, 1, 3))
    first, corner, tq, table = pl.pallas_call(
        outer_kernel,
        out_shape=(
            jax.ShapeDtypeStruct((3 * COLS, NTIME), BF),
            jax.ShapeDtypeStruct((COLS, NTIME), BF),
            jax.ShapeDtypeStruct((NQ * NJ, NTIME), BF),
            jax.ShapeDtypeStruct((24, NJ), F32),
        ),
        in_specs=[HBM] * 6,
        out_specs=(VMEM,) * 4,
        scratch_shapes=[
            pltpu.VMEM((NJ, NS), BF),
            pltpu.VMEM((2, 3, 2, TR), jnp.int32),
            pltpu.VMEM((2, 2, TR), BF),
            pltpu.VMEM((NC, NTIME), jnp.int32),
            pltpu.SMEM((2, 2, 9), jnp.int32),
            pltpu.SMEM((NC,), F32),
            pltpu.SemaphoreType.DMA((6,)),
            pltpu.VMEM((NJ, NTIME), BF),
            pltpu.VMEM((NJ, NREACH * NTIME), BF),
            pltpu.VMEM((4 * COLS, NJ), BF),
        ],
        compiler_params=PARAMS,
        name="outer",
    )(*(in_hbm(x) for x in (traces.reshape(NJ, NS), geom, trace_weight, traveltime, aperture, class_weight)))
    from_first = lax.ppermute(first, "gx", swaps("gx", False))
    from_corner = lax.ppermute(corner, "gx", swaps("gx", True))
    second, slow = later_tiles(side_kernel, (BF, F32), tq, table)
    from_second = lax.ppermute(second, "gx", swaps("gx", True))
    slow = slow + from_first[:COLS].astype(F32) + from_corner.astype(F32)
    far = lax.ppermute(slow.astype(BF), "gy", swaps("gy", True))
    (own,) = later_tiles(own_kernel, (F32,), tq, table)
    own = own + from_first[COLS:].astype(F32) + from_second.astype(F32)
    near = lax.ppermute(own[COLS:], "gy", swaps("gy", False))
    image = own[:COLS] + near + far.astype(F32)
    return image.reshape(PX, PY, NTIME)


def solution(mesh):
    return jax.shard_map(
        per_device,
        mesh=mesh,
        in_specs=(
            P("gx", "gy", None, None),
            P("gx", "gy", None),
            P("gx", "gy", None, None),
            P("gx", "gy", None),
            P(),
            P(),
        ),
        out_specs=P("gx", "gy", None),
        check_vma=False,
    )
```

```python
import jax
import jax.numpy as jnp
from jax import lax
from jax.experimental import pallas as pl
from jax.experimental.pallas import tpu as pltpu
from jax.sharding import PartitionSpec as P


NS = 256
NTIME = 256
PX = 16
PY = 8
DSTEP = 8
TR = 128
NH = 8
NC = 14
COLS = PX * PY
NJ = 4 * TR
NQ = (2 * PX - 1 + 2 * PY - 1) // DSTEP + 1
LEVEL = 129.0
BF = jnp.bfloat16
F32 = jnp.float32


NB = 4
HALF = COLS // 2
NREACH = NH + NQ - 1
PICK_UNROLL = 8
ROW_X, ROW_Y, ROW_SCALE, ROW_LIVE = 0, 1, 2, 2 + NQ


def row_of(parts):
    return jnp.concatenate(parts, axis=1)


def blocks(piece):
    return row_of([piece(i, k) for i in range(2) for k in range(2)])


def down(piece, rows):
    return jnp.concatenate([piece] * (rows // 16), axis=0)


def partners():
    dx = 1 - 2 * (lax.axis_index("gx") % 2)
    dy = 1 - 2 * (lax.axis_index("gy") % 2)
    return dx, dy


def inline_distance(first, count, mx):
    px = (lax.broadcasted_iota(jnp.int32, (count, NJ), 0) + first).astype(F32)
    ax = (2.0 * jnp.abs(px - mx) - (DSTEP - 1)) * (0.5 / DSTEP)
    ax = jnp.broadcast_to(ax[:, None, :], (count, PY, NJ)).reshape(count * PY, NJ)
    return ax.astype(BF)


def halves(dx):
    near = (PX // 4) * (1 - dx)
    return near, PX // 2 - near


def near_and_far(dx, mx):
    return [inline_distance(PX * dx + half, PX // 2, mx) for half in halves(dx)]


def half_rows(n, half):
    return pl.ds(pl.multiple_of(n * COLS + half * PY, HALF), HALF)


def crossline_distance(dy, my):
    py = (lax.broadcasted_iota(jnp.int32, (16, NJ), 0) % PY + PY * dy).astype(F32)
    return (jnp.abs(py - my) * (1.0 / DSTEP)).astype(BF)


def class_scales(h, w, cw_ref):
    scales = []
    for q in range(NQ):
        cw = jnp.full(h.shape, cw_ref[q], F32)
        for k in range(1, NH):
            cw = jnp.where(h == k, cw_ref[k + q], cw)
        scales.append((w * cw).astype(BF).astype(F32))
    return scales


def live_row(ap_ref, dx, dy):
    entry = (dx + 1) * 3 + dy + 1
    return blocks(lambda i, k: jnp.full((1, TR), ap_ref[i, k, entry].astype(F32), F32))


def amplitude(level, scales, lives, q):
    rows = level.shape[0] // len(lives)
    scale = [down(jnp.broadcast_to(scales[q] * live, (16, NJ)).astype(BF), rows) for live in lives]
    return jnp.where(level == jnp.asarray(LEVEL + q, BF), jnp.concatenate(scale, axis=0), jnp.zeros((), BF))


def stacked(tq_ref, level, scales, lives, reach):
    out = jnp.zeros((level.shape[0], NTIME), F32)
    for q in reach:
        a = amplitude(level, scales, lives, q)
        out = out + jnp.dot(a, tq_ref[q * NJ : (q + 1) * NJ, :], preferred_element_type=F32)
    return out


def levels(ax, ay):
    return ax + down(ay, ax.shape[0]) + jnp.asarray(LEVEL, BF)


def outer_kernel(
    traces_hbm, geom_hbm, w_hbm, tt_hbm, ap_hbm, cw_hbm,
    first_ref, corner_ref, tq_ref, table_ref,
    traces_ref, geom_ref, w_ref, tt_ref, ap_ref, cw_ref, sems, class_ref, t_ref, level_ref,
):
    pairs = (
        (traces_hbm, traces_ref), (geom_hbm, geom_ref), (tt_hbm, tt_ref),
        (w_hbm, w_ref), (cw_hbm, cw_ref), (ap_hbm, ap_ref),
    )
    copies = [pltpu.make_async_copy(a, b, sems.at[n]) for n, (a, b) in enumerate(pairs)]
    for copy in copies:
        copy.start()
    dx, dy = partners()
    for copy in copies[1:]:
        copy.wait()
    h = blocks(lambda i, k: geom_ref[i, 2, k : k + 1, :])
    mx = blocks(lambda i, k: geom_ref[i, 0, k : k + 1, :] & (PX - 1)).astype(F32)
    my = blocks(lambda i, k: geom_ref[i, 1, k : k + 1, :] & (PY - 1)).astype(F32)
    w = blocks(lambda i, k: w_ref[i, k : k + 1, :]).astype(F32)
    table_ref[ROW_X : ROW_X + 1, :] = mx
    table_ref[ROW_Y : ROW_Y + 1, :] = my
    for q, scale in enumerate(class_scales(h, w, cw_ref)):
        table_ref[ROW_SCALE + q : ROW_SCALE + q + 1, :] = scale
    tiles = outer_tiles(dx, dy)
    for n, (tx, ty) in enumerate(inner_tiles(dx, dy) + tiles):
        table_ref[ROW_LIVE + n : ROW_LIVE + n + 1, :] = live_row(ap_ref, tx, ty)
    hf = h.astype(F32)
    for b in range(NB):
        column = jnp.broadcast_to(hf[:, b * TR : (b + 1) * TR], (TR, TR)).T
        class_ref[b * TR : (b + 1) * TR, :] = jnp.concatenate([column, column], axis=1).astype(BF)
    ays = [crossline_distance(t, my) for t in (-dy, 0, dy)]
    axs = [near_and_far(t, mx) for t in (dx, -dx)]
    which = ((0, 0), (0, 1), (0, 2), (1, 0))
    for half in range(2):
        for n, (x, y) in enumerate(which):
            at = (4 * half + n) * HALF
            level_ref[at : at + HALF, :] = levels(axs[x][half], ays[y])
    copies[0].wait()
    sample = lax.broadcasted_iota(jnp.int32, (NS, NTIME), 0).astype(F32).astype(BF)
    for c in range(NREACH):
        quarter = tt_ref[c : c + 1, :]
        whole = jnp.minimum(quarter >> 2, NS).astype(F32)
        part = (quarter & 3).astype(F32) * 0.25
        whole = down(jnp.broadcast_to(whole, (16, NTIME)).astype(BF), NS)
        part = down(jnp.broadcast_to(part, (16, NTIME)).astype(BF), NS)
        away = jnp.abs((sample - whole) - part)
        interp = jnp.maximum(jnp.asarray(1.0, BF) - away, jnp.asarray(0.0, BF))
        lanes = slice(c * NTIME, (c + 1) * NTIME)
        for n in range(2):
            rows = slice(n * (NJ // 2), (n + 1) * (NJ // 2))
            t_ref[rows, lanes] = jnp.dot(traces_ref[rows, :], interp, preferred_element_type=F32).astype(BF)

    def pick(n, carry):
        rows = pl.ds(pl.multiple_of(n * 16, 16), 16)
        k = class_ref[rows, :]
        bit4 = k >= jnp.asarray(4.0, BF)
        k = jnp.where(bit4, k - jnp.asarray(4.0, BF), k)
        bit2 = k >= jnp.asarray(2.0, BF)
        k = jnp.where(bit2, k - jnp.asarray(2.0, BF), k)
        bit1 = k >= jnp.asarray(1.0, BF)
        t = [t_ref[rows, c * NTIME : (c + 1) * NTIME] for c in range(NREACH)]
        for bit, shift in ((bit1, 1), (bit2, 2), (bit4, 4)):
            t = [jnp.where(bit, t[c + shift], t[c]) for c in range(len(t) - shift)]
        for q in range(NQ):
            tq_ref[pl.ds(pl.multiple_of(q * NJ + n * 16, 16), 16), :] = t[q]
        return carry

    lax.fori_loop(0, NJ // 16, pick, 0, unroll=PICK_UNROLL)
    _, _, scales, lives = table_rows(table_ref)
    lives = lives[len(inner_tiles(dx, dy)) :]
    place = lax.axis_index("gx")
    at_end = (place == 0) | (place == lax.axis_size("gx") - 1)

    def stack(count):
        near = stacked(tq_ref, level_ref[: count * HALF, :], scales, lives[:count], range(NQ - 1)).astype(BF)
        far_rows = level_ref[4 * HALF : (4 + count) * HALF, :]
        far = stacked(tq_ref, far_rows, scales, lives[:count], range(1, NQ)).astype(BF)
        for out, half in zip((near, far), halves(dx), strict=True):
            for n in range(3):
                first_ref[half_rows(n, half), :] = out[n * HALF : (n + 1) * HALF]
        if count == 4:
            for out, half in zip((near, far), halves(-dx), strict=True):
                corner_ref[half_rows(0, half), :] = out[3 * HALF :]

    @pl.when(at_end)
    def end():
        stack(3)
        corner_ref[...] = jnp.zeros_like(corner_ref)

    @pl.when(jnp.logical_not(at_end))
    def middle():
        stack(4)


def outer_tiles(dx, dy):
    return ((dx, -dy), (dx, 0), (dx, dy), (-dx, -dy))


def inner_tiles(dx, dy):
    return ((-dx, 0), (-dx, dy), (0, 0), (0, dy), (0, -dy))


def table_rows(table_ref):
    mx, my = table_ref[ROW_X : ROW_X + 1, :], table_ref[ROW_Y : ROW_Y + 1, :]
    scales = [table_ref[ROW_SCALE + q : ROW_SCALE + q + 1, :] for q in range(NQ)]
    return mx, my, scales, [table_ref[ROW_LIVE + n : ROW_LIVE + n + 1, :] for n in range(9)]


def side_kernel(tq_ref, table_ref, second_ref, slow_ref):
    dx, dy = partners()
    mx, my, scales, lives = table_rows(table_ref)
    axs = near_and_far(-dx, mx)
    ays = [crossline_distance(ty, my) for ty in (0, dy)]
    for ax, half, reach in zip(axs, halves(-dx), (range(NQ - 1), range(1, NQ)), strict=True):
        level = jnp.concatenate([levels(ax, ay) for ay in ays], axis=0)
        out = stacked(tq_ref, level, scales, lives[:2], reach).astype(BF)
        for n in range(2):
            second_ref[half_rows(n, half), :] = out[n * HALF : (n + 1) * HALF]
    level = levels(inline_distance(0, PX, mx), crossline_distance(-dy, my))
    slow_ref[...] = stacked(tq_ref, level, scales, lives[4:5], range(4))


def own_kernel(tq_ref, table_ref, own_ref):
    _, dy = partners()
    mx, my, scales, lives = table_rows(table_ref)
    ax = inline_distance(0, PX, mx)
    for n, ty in enumerate((0, dy)):
        level = levels(ax, crossline_distance(ty, my))
        own_ref[n * COLS : (n + 1) * COLS, :] = stacked(tq_ref, level, scales, lives[2 + n : 3 + n], range(3 + n))


def swaps(axis, odd):
    n = lax.axis_size(axis)
    lower = range(1 if odd else 0, n - 1, 2)
    return [p for i in lower for p in ((i, i + 1), (i + 1, i))]


HBM = pl.BlockSpec(memory_space=pltpu.HBM)
VMEM = pl.BlockSpec(memory_space=pltpu.VMEM)
LATER_COST = pl.CostEstimate(flops=2 * 7 * COLS * NJ * NTIME, bytes_accessed=1 << 21, transcendentals=0)
PARAMS = pltpu.CompilerParams(vmem_limit_bytes=24 << 20)


def in_hbm(x):
    return pltpu.with_memory_space_constraint(x, pltpu.HBM)


def later_tiles(kernel, dtypes, tq, table):
    return pl.pallas_call(
        kernel,
        out_shape=tuple(jax.ShapeDtypeStruct(((2 - n) * COLS, NTIME), t) for n, t in enumerate(dtypes)),
        in_specs=[VMEM] * 2,
        out_specs=(VMEM,) * len(dtypes),
        compiler_params=PARAMS,
        cost_estimate=LATER_COST,
    )(tq, table)


def per_device(traces, aperture, geometry, trace_weight, class_weight, traveltime):
    geom = jnp.transpose(geometry, (0, 2, 1, 3))
    first, corner, tq, table = pl.pallas_call(
        outer_kernel,
        out_shape=(
            jax.ShapeDtypeStruct((3 * COLS, NTIME), BF),
            jax.ShapeDtypeStruct((COLS, NTIME), BF),
            jax.ShapeDtypeStruct((NQ * NJ, NTIME), BF),
            jax.ShapeDtypeStruct((24, NJ), F32),
        ),
        in_specs=[HBM] * 6,
        out_specs=(VMEM,) * 4,
        scratch_shapes=[
            pltpu.VMEM((NJ, NS), BF),
            pltpu.VMEM((2, 3, 2, TR), jnp.int32),
            pltpu.VMEM((2, 2, TR), BF),
            pltpu.VMEM((NC, NTIME), jnp.int32),
            pltpu.SMEM((2, 2, 9), jnp.int32),
            pltpu.SMEM((NC,), F32),
            pltpu.SemaphoreType.DMA((6,)),
            pltpu.VMEM((NJ, NTIME), BF),
            pltpu.VMEM((NJ, NREACH * NTIME), BF),
            pltpu.VMEM((4 * COLS, NJ), BF),
        ],
        compiler_params=PARAMS,
        name="outer",
    )(*(in_hbm(x) for x in (traces.reshape(NJ, NS), geom, trace_weight, traveltime, aperture, class_weight)))
    from_first = lax.ppermute(first, "gx", swaps("gx", False))
    from_corner = lax.ppermute(corner, "gx", swaps("gx", True))
    second, slow = later_tiles(side_kernel, (BF, F32), tq, table)
    from_second = lax.ppermute(second, "gx", swaps("gx", True))
    slow = slow + from_first[:COLS].astype(F32) + from_corner.astype(F32)
    far = lax.ppermute(slow.astype(BF), "gy", swaps("gy", True))
    (own,) = later_tiles(own_kernel, (F32,), tq, table)
    own = own + from_first[COLS:].astype(F32) + from_second.astype(F32)
    near = lax.ppermute(own[COLS:], "gy", swaps("gy", False))
    image = own[:COLS] + near + far.astype(F32)
    return image.reshape(PX, PY, NTIME)


def solution(mesh):
    return jax.shard_map(
        per_device,
        mesh=mesh,
        in_specs=(
            P("gx", "gy", None, None),
            P("gx", "gy", None),
            P("gx", "gy", None, None),
            P("gx", "gy", None),
            P(),
            P(),
        ),
        out_specs=P("gx", "gy", None),
        check_vma=False,
    )
```

```python
import jax
import jax.numpy as jnp
from jax import lax
from jax.experimental import pallas as pl
from jax.experimental.pallas import tpu as pltpu
from jax.sharding import PartitionSpec as P


NS = 256
NTIME = 256
PX = 16
PY = 8
DSTEP = 8
TR = 128
NH = 8
NC = 14
COLS = PX * PY
NJ = 4 * TR
NQ = (2 * PX - 1 + 2 * PY - 1) // DSTEP + 1
LEVEL = 129.0
BF = jnp.bfloat16
F32 = jnp.float32


NB = 4
HALF = COLS // 2
NREACH = NH + NQ - 1
PICK_UNROLL = 8
ROW_X, ROW_Y, ROW_SCALE, ROW_LIVE = 0, 1, 2, 2 + NQ


def row_of(parts):
    return jnp.concatenate(parts, axis=1)


def blocks(piece):
    return row_of([piece(i, k) for i in range(2) for k in range(2)])


def down(piece, rows):
    return jnp.concatenate([piece] * (rows // 16), axis=0)


def partners():
    dx = 1 - 2 * (lax.axis_index("gx") % 2)
    dy = 1 - 2 * (lax.axis_index("gy") % 2)
    return dx, dy


def inline_distance(first, count, mx):
    px = (lax.broadcasted_iota(jnp.int32, (count, NJ), 0) + first).astype(F32)
    ax = (2.0 * jnp.abs(px - mx) - (DSTEP - 1)) * (0.5 / DSTEP)
    ax = jnp.broadcast_to(ax[:, None, :], (count, PY, NJ)).reshape(count * PY, NJ)
    return ax.astype(BF)


def halves(dx):
    near = (PX // 4) * (1 - dx)
    return near, PX // 2 - near


def near_and_far(dx, mx):
    return [inline_distance(PX * dx + half, PX // 2, mx) for half in halves(dx)]


def half_rows(n, half):
    return pl.ds(pl.multiple_of(n * COLS + half * PY, HALF), HALF)


def crossline_distance(dy, my):
    py = (lax.broadcasted_iota(jnp.int32, (16, NJ), 0) % PY + PY * dy).astype(F32)
    return (jnp.abs(py - my) * (1.0 / DSTEP)).astype(BF)


def class_scales(h, w, cw_ref):
    scales = []
    for q in range(NQ):
        cw = jnp.full(h.shape, cw_ref[q], F32)
        for k in range(1, NH):
            cw = jnp.where(h == k, cw_ref[k + q], cw)
        scales.append((w * cw).astype(BF).astype(F32))
    return scales


def live_row(ap_ref, dx, dy):
    entry = (dx + 1) * 3 + dy + 1
    return blocks(lambda i, k: jnp.full((1, TR), ap_ref[i, k, entry].astype(F32), F32))


def amplitude(level, scales, lives, q):
    rows = level.shape[0] // len(lives)
    scale = [down(jnp.broadcast_to(scales[q] * live, (16, NJ)).astype(BF), rows) for live in lives]
    return jnp.where(level == jnp.asarray(LEVEL + q, BF), jnp.concatenate(scale, axis=0), jnp.zeros((), BF))


def stacked(tq_ref, level, scales, lives, reach):
    out = jnp.zeros((level.shape[0], NTIME), F32)
    for q in reach:
        a = amplitude(level, scales, lives, q)
        out = out + jnp.dot(a, tq_ref[q * NJ : (q + 1) * NJ, :], preferred_element_type=F32)
    return out


def levels(ax, ay):
    return ax + down(ay, ax.shape[0]) + jnp.asarray(LEVEL, BF)


def outer_kernel(
    traces_hbm, geom_hbm, w_hbm, tt_hbm, ap_hbm, cw_hbm,
    first_ref, corner_ref, second_ref, tq_ref, table_ref,
    traces_ref, geom_ref, w_ref, tt_ref, ap_ref, cw_ref, sems, class_ref, t_ref, level_ref,
):
    pairs = (
        (traces_hbm, traces_ref), (geom_hbm, geom_ref), (tt_hbm, tt_ref),
        (w_hbm, w_ref), (cw_hbm, cw_ref), (ap_hbm, ap_ref),
    )
    copies = [pltpu.make_async_copy(a, b, sems.at[n]) for n, (a, b) in enumerate(pairs)]
    for copy in copies:
        copy.start()
    dx, dy = partners()
    for copy in copies[1:]:
        copy.wait()
    h = blocks(lambda i, k: geom_ref[i, 2, k : k + 1, :])
    mx = blocks(lambda i, k: geom_ref[i, 0, k : k + 1, :] & (PX - 1)).astype(F32)
    my = blocks(lambda i, k: geom_ref[i, 1, k : k + 1, :] & (PY - 1)).astype(F32)
    w = blocks(lambda i, k: w_ref[i, k : k + 1, :]).astype(F32)
    table_ref[ROW_X : ROW_X + 1, :] = mx
    table_ref[ROW_Y : ROW_Y + 1, :] = my
    for q, scale in enumerate(class_scales(h, w, cw_ref)):
        table_ref[ROW_SCALE + q : ROW_SCALE + q + 1, :] = scale
    tiles = outer_tiles(dx, dy)
    for n, (tx, ty) in enumerate(inner_tiles(dx, dy) + tiles):
        table_ref[ROW_LIVE + n : ROW_LIVE + n + 1, :] = live_row(ap_ref, tx, ty)
    hf = h.astype(F32)
    for b in range(NB):
        column = jnp.broadcast_to(hf[:, b * TR : (b + 1) * TR], (TR, TR)).T
        class_ref[b * TR : (b + 1) * TR, :] = jnp.concatenate([column, column], axis=1).astype(BF)
    ays = [crossline_distance(t, my) for t in (-dy, 0, dy)]
    axs = [near_and_far(t, mx) for t in (dx, -dx)]
    which = ((0, 0), (0, 1), (0, 2), (1, 0))
    for half in range(2):
        for n, (x, y) in enumerate(which):
            at = (4 * half + n) * HALF
            level_ref[at : at + HALF, :] = levels(axs[x][half], ays[y])
    copies[0].wait()
    sample = lax.broadcasted_iota(jnp.int32, (NS, NTIME), 0).astype(F32).astype(BF)
    for c in range(NREACH):
        quarter = tt_ref[c : c + 1, :]
        whole = jnp.minimum(quarter >> 2, NS).astype(F32)
        part = (quarter & 3).astype(F32) * 0.25
        whole = down(jnp.broadcast_to(whole, (16, NTIME)).astype(BF), NS)
        part = down(jnp.broadcast_to(part, (16, NTIME)).astype(BF), NS)
        away = jnp.abs((sample - whole) - part)
        interp = jnp.maximum(jnp.asarray(1.0, BF) - away, jnp.asarray(0.0, BF))
        lanes = slice(c * NTIME, (c + 1) * NTIME)
        for n in range(2):
            rows = slice(n * (NJ // 2), (n + 1) * (NJ // 2))
            t_ref[rows, lanes] = jnp.dot(traces_ref[rows, :], interp, preferred_element_type=F32).astype(BF)

    def pick(n, carry):
        rows = pl.ds(pl.multiple_of(n * 16, 16), 16)
        k = class_ref[rows, :]
        bit4 = k >= jnp.asarray(4.0, BF)
        k = jnp.where(bit4, k - jnp.asarray(4.0, BF), k)
        bit2 = k >= jnp.asarray(2.0, BF)
        k = jnp.where(bit2, k - jnp.asarray(2.0, BF), k)
        bit1 = k >= jnp.asarray(1.0, BF)
        t = [t_ref[rows, c * NTIME : (c + 1) * NTIME] for c in range(NREACH)]
        for bit, shift in ((bit1, 1), (bit2, 2), (bit4, 4)):
            t = [jnp.where(bit, t[c + shift], t[c]) for c in range(len(t) - shift)]
        for q in range(NQ):
            tq_ref[pl.ds(pl.multiple_of(q * NJ + n * 16, 16), 16), :] = t[q]
        return carry

    lax.fori_loop(0, NJ // 16, pick, 0, unroll=PICK_UNROLL)
    _, _, scales, lives = table_rows(table_ref)
    lives = lives[len(inner_tiles(dx, dy)) :]
    place = lax.axis_index("gx")
    at_end = (place == 0) | (place == lax.axis_size("gx") - 1)

    def stack(count):
        near = stacked(tq_ref, level_ref[: count * HALF, :], scales, lives[:count], range(NQ - 1)).astype(BF)
        far_rows = level_ref[4 * HALF : (4 + count) * HALF, :]
        far = stacked(tq_ref, far_rows, scales, lives[:count], range(1, NQ)).astype(BF)
        for out, half in zip((near, far), halves(dx), strict=True):
            for n in range(3):
                first_ref[half_rows(n, half), :] = out[n * HALF : (n + 1) * HALF]
        if count == 4:
            for out, half in zip((near, far), halves(-dx), strict=True):
                corner_ref[half_rows(0, half), :] = out[3 * HALF :]

    @pl.when(at_end)
    def end():
        stack(3)
        corner_ref[...] = jnp.zeros_like(corner_ref)
        second_ref[...] = jnp.zeros_like(second_ref)

    @pl.when(jnp.logical_not(at_end))
    def middle():
        stack(4)
        side_tiles(tq_ref, table_ref, second_ref)


def outer_tiles(dx, dy):
    return ((dx, -dy), (dx, 0), (dx, dy), (-dx, -dy))


def inner_tiles(dx, dy):
    return ((-dx, 0), (-dx, dy), (0, 0), (0, dy), (0, -dy))


def table_rows(table_ref):
    mx, my = table_ref[ROW_X : ROW_X + 1, :], table_ref[ROW_Y : ROW_Y + 1, :]
    scales = [table_ref[ROW_SCALE + q : ROW_SCALE + q + 1, :] for q in range(NQ)]
    return mx, my, scales, [table_ref[ROW_LIVE + n : ROW_LIVE + n + 1, :] for n in range(9)]


def side_tiles(tq_ref, table_ref, second_ref):
    dx, dy = partners()
    mx, my, scales, lives = table_rows(table_ref)
    axs = near_and_far(-dx, mx)
    ays = [crossline_distance(ty, my) for ty in (0, dy)]
    for ax, half, reach in zip(axs, halves(-dx), (range(NQ - 1), range(1, NQ)), strict=True):
        level = jnp.concatenate([levels(ax, ay) for ay in ays], axis=0)
        out = stacked(tq_ref, level, scales, lives[:2], reach).astype(BF)
        for n in range(2):
            second_ref[half_rows(n, half), :] = out[n * HALF : (n + 1) * HALF]


def slow_kernel(tq_ref, table_ref, slow_ref):
    _, dy = partners()
    mx, my, scales, lives = table_rows(table_ref)
    level = levels(inline_distance(0, PX, mx), crossline_distance(-dy, my))
    slow_ref[...] = stacked(tq_ref, level, scales, lives[4:5], range(4))


def own_kernel(tq_ref, table_ref, own_ref):
    _, dy = partners()
    mx, my, scales, lives = table_rows(table_ref)
    ax = inline_distance(0, PX, mx)
    for n, ty in enumerate((0, dy)):
        level = levels(ax, crossline_distance(ty, my))
        own_ref[n * COLS : (n + 1) * COLS, :] = stacked(tq_ref, level, scales, lives[2 + n : 3 + n], range(3 + n))


def swaps(axis, odd):
    n = lax.axis_size(axis)
    lower = range(1 if odd else 0, n - 1, 2)
    return [p for i in lower for p in ((i, i + 1), (i + 1, i))]


HBM = pl.BlockSpec(memory_space=pltpu.HBM)
VMEM = pl.BlockSpec(memory_space=pltpu.VMEM)
LATER_COST = pl.CostEstimate(flops=2 * 7 * COLS * NJ * NTIME, bytes_accessed=1 << 21, transcendentals=0)
PARAMS = pltpu.CompilerParams(vmem_limit_bytes=24 << 20)


def in_hbm(x):
    return pltpu.with_memory_space_constraint(x, pltpu.HBM)


def later_tiles(kernel, tiles, tq, table):
    return pl.pallas_call(
        kernel,
        out_shape=jax.ShapeDtypeStruct((tiles * COLS, NTIME), F32),
        in_specs=[VMEM] * 2,
        out_specs=VMEM,
        compiler_params=PARAMS,
        cost_estimate=LATER_COST,
    )(tq, table)


def per_device(traces, aperture, geometry, trace_weight, class_weight, traveltime):
    geom = jnp.transpose(geometry, (0, 2, 1, 3))
    first, corner, second, tq, table = pl.pallas_call(
        outer_kernel,
        out_shape=(
            jax.ShapeDtypeStruct((3 * COLS, NTIME), BF),
            jax.ShapeDtypeStruct((COLS, NTIME), BF),
            jax.ShapeDtypeStruct((2 * COLS, NTIME), BF),
            jax.ShapeDtypeStruct((NQ * NJ, NTIME), BF),
            jax.ShapeDtypeStruct((24, NJ), F32),
        ),
        in_specs=[HBM] * 6,
        out_specs=(VMEM,) * 5,
        scratch_shapes=[
            pltpu.VMEM((NJ, NS), BF),
            pltpu.VMEM((2, 3, 2, TR), jnp.int32),
            pltpu.VMEM((2, 2, TR), BF),
            pltpu.VMEM((NC, NTIME), jnp.int32),
            pltpu.SMEM((2, 2, 9), jnp.int32),
            pltpu.SMEM((NC,), F32),
            pltpu.SemaphoreType.DMA((6,)),
            pltpu.VMEM((NJ, NTIME), BF),
            pltpu.VMEM((NJ, NREACH * NTIME), BF),
            pltpu.VMEM((4 * COLS, NJ), BF),
        ],
        compiler_params=PARAMS,
        name="outer",
    )(*(in_hbm(x) for x in (traces.reshape(NJ, NS), geom, trace_weight, traveltime, aperture, class_weight)))
    from_first = lax.ppermute(first, "gx", swaps("gx", False))
    from_corner = lax.ppermute(corner, "gx", swaps("gx", True))
    slow = later_tiles(slow_kernel, 1, tq, table)
    from_second = lax.ppermute(second, "gx", swaps("gx", True))
    slow = slow + from_first[:COLS].astype(F32) + from_corner.astype(F32)
    far = lax.ppermute(slow.astype(BF), "gy", swaps("gy", True))
    own = later_tiles(own_kernel, 2, tq, table)
    own = own + from_first[COLS:].astype(F32) + from_second.astype(F32)
    near = lax.ppermute(own[COLS:], "gy", swaps("gy", False))
    image = own[:COLS] + near + far.astype(F32)
    return image.reshape(PX, PY, NTIME)


def solution(mesh):
    return jax.shard_map(
        per_device,
        mesh=mesh,
        in_specs=(
            P("gx", "gy", None, None),
            P("gx", "gy", None),
            P("gx", "gy", None, None),
            P("gx", "gy", None),
            P(),
            P(),
        ),
        out_specs=P("gx", "gy", None),
        check_vma=False,
    )
```
